128 devices in a mesh: seq: 64 (over y_lo, x, z, core), head: 2 (over y_hi).
Axes of the slice: x: 4, y: 4 (y_hi: 2, y_lo: 2; y = y_hi * 2 + y_lo), z: 4, core: 2. Of those that a mesh axis runs over, the one named last changes fastest.
Arguments:
- queries: bfloat16 [32768, 768], P('seq', 'head'), may hold values from -7 to 7
- keys: bfloat16 [32768, 768], P('seq', 'head'), may hold values from -7 to 7
- values: bfloat16 [32768, 768], P('seq', 'head'), may hold values from -6 to 6
- w_out: bfloat16 [768, 768], P('head'), may hold values from -0.21875 to 0.21875
- d_out: bfloat16 [32768, 768], P('seq', 'head'), may hold values from -16 to 16
- slide_lengths: int32 [4], replicated, may hold values from 1 to 16384, 32768 in all
Outputs:
- out: bfloat16 [32768, 768], P('seq', 'head')
- d_queries: bfloat16 [32768, 768], P('seq', 'head')
- d_keys: bfloat16 [32768, 768], P('seq', 'head')
- d_values: bfloat16 [32768, 768], P('seq', 'head')
- d_w_out: float32 [768, 768], P('head', 'seq')
The draws below stay inside these ranges and needn't reach their ends.
Inputs may be any that keep to these rules, and one draw needn't show every extreme that they name: `slide_lengths`: the lengths sum to 32768 and the longest is exactly 16384.
All inputs are finite; a program needn't handle non-finite values.
Results may differ from the reference program's by a relative error of at most 0.012.
Values may be sent and summed in bfloat16 or wider, within the bound.
A program may use at most 128 MiB of HBM per device.

```python
import math
import jax
import jax.numpy as jnp
import numpy as np
from jax import lax

D = 768
H = 16
TOK_DEV = 512
SLIDES = 4
TOKENS = 32768
LONGEST = 16384
N_SEQ = 64


def paired(key):
    base = jax.random.fold_in(key, 7)
    key_q, key_k = jax.random.split(base, 2)
    first = jnp.clip(1.4 * jax.random.normal(key_q, (TOKENS, D), jnp.float32), -5.6, 5.6)
    second = jnp.clip(1.4 * jax.random.normal(key_k, (TOKENS, D), jnp.float32), -5.6, 5.6)
    return (first, second)


def draw_queries(key, part):
    return paired(key)[0].astype(jnp.bfloat16)


def draw_keys(key, part):
    return paired(key)[1].astype(jnp.bfloat16)


def raised(drawn, key, source, target, parts, factor):
    def block_of(dim):
        return (jnp.arange(drawn.shape[dim]) // (drawn.shape[dim] // parts)).reshape((-1,) + (1,) * (drawn.ndim - 1 - dim))

    first = jax.random.permutation(key, parts)[block_of(target)]
    other_side = (block_of(target) + parts // 2) % parts
    return jnp.where((block_of(source) == first) | (block_of(source) == other_side), factor * drawn, drawn)


def block_levels(own_key, dims, shards, low, high):
    def one(position, shards_of):
        steps = jax.random.uniform(jax.random.fold_in(jax.random.fold_in(own_key, 6), position), (shards_of,), jnp.float32, low / len(shards), high / len(shards))
        return jnp.repeat(jnp.exp(steps), dims[position] // shards_of).reshape((-1,) + (1,) * (len(dims) - position - 1))

    loudness = one(*shards[0])
    for cut in shards[1:]:
        loudness = loudness * one(*cut)
    return loudness


def length_profile(number_of, total, reach, slope):
    loads = [(1 << 20) // math.isqrt(grade ** slope) + 1 for grade in range(2, number_of + 1)]
    rest, holding = total - reach - (number_of - 1), [1] * (number_of - 1)
    while rest > 0:
        movable = [i for i in range(number_of - 1) if holding[i] < reach]
        pool, remaining = sum([loads[i] for i in movable]), rest
        for i in movable:
            extra = min(reach - holding[i], max(1, remaining * loads[i] // pool), rest)
            holding[i] = holding[i] + extra
            rest = rest - extra
    return np.array([reach] + holding)


def uneven_parts(own_key, count, total, limit, skew):
    if count == 2:
        one = jax.random.randint(own_key, (), max(1, total - limit), min(limit, total - 1) + 1)
        return jnp.stack([one, total - one])
    tallies = jnp.asarray(length_profile(count, total, limit, skew), jnp.int32)
    pairs = (count - 1) // 2
    giver, sink = tallies[1:1 + 2 * pairs:2], tallies[2:2 + 2 * pairs:2]
    room = jnp.minimum(giver - 1, limit - sink)
    moved = jax.random.randint(jax.random.fold_in(own_key, 1), (pairs,), 0, 1 << 20) % (room + 1)
    tallies = tallies.at[1:1 + 2 * pairs:2].set(giver - moved).at[2:2 + 2 * pairs:2].set(sink + moved)
    return tallies[jax.random.permutation(jax.random.fold_in(own_key, 2), count)]


def normal_values(own_key, extent, scale, most, cuts=(), kind=jnp.bfloat16):
    values = jax.random.normal(own_key, extent, jnp.float32) * scale
    if len(cuts) > 0:
        values = block_levels(own_key, extent, cuts, -0.22, 0.18) * values
    return jnp.clip(values, min=-most, max=most).astype(kind)


def noise_with(key, extent, scale, reach, cuts, heavy, kind=jnp.bfloat16):
    result = scale * jax.random.normal(key, extent, jnp.float32)
    if cuts:
        result = result * block_levels(key, extent, cuts, -0.22, 0.18)
    return jnp.clip(raised(result, jax.random.fold_in(key, 3), *heavy), -reach, reach).astype(kind)


def setup_inputs(seed: int = 0) -> dict:
    streams_of = jax.random.split(jax.random.key(seed), 7)
    queries = draw_queries(jax.random.fold_in(streams_of[6], 71), 0)
    keys = draw_keys(jax.random.fold_in(streams_of[6], 71), 0)
    values = normal_values(streams_of[2], (TOKENS, D), 1.0, 6.0, ((0, 64), (1, 2)))
    w_out = normal_values(streams_of[3], (D, D), D ** -0.5, 0.21875, ((0, 2),))
    d_out = noise_with(streams_of[4], (TOKENS, D), 1.0, 16.0, ((0, 64), (1, 2)), (0, 1, 64, 4.0))
    slide_lengths = uneven_parts(streams_of[5], SLIDES, TOKENS, LONGEST, 2).astype(jnp.int32)
    return dict(queries=queries, keys=keys, values=values, w_out=w_out, d_out=d_out, slide_lengths=slide_lengths)


NEG = -1.0e30


def slide_ids(positions, starts):
    return jnp.sum((positions[..., None] >= starts).astype(jnp.int32), axis=-1).astype(jnp.int32)


def select(array, dilation, heads):
    segments = TOKENS // (TOK_DEV * dilation)
    shaped = array.reshape((segments, TOK_DEV, dilation, H) + array.shape[2:])
    return shaped[:, :, heads % dilation, heads]


def place(array, dilation, heads, fill):
    segments = array.shape[0]
    shaped = jnp.full((segments, TOK_DEV, dilation, H) + array.shape[3:], fill, array.dtype)
    shaped = shaped.at[:, :, heads % dilation, heads].set(array)
    return shaped.reshape((TOKENS, H) + array.shape[3:])


def to_bf16_f32(array):
    return lax.optimization_barrier(array.astype(jnp.bfloat16)).astype(jnp.float32)


def segment_forward(q_rows, k_rows, v_rows, row_ids, scale):
    scores = jnp.einsum("qhd,khd->hqk", q_rows.astype(jnp.float32), k_rows.astype(jnp.float32)) * scale
    allowed = row_ids.T[:, :, None] == row_ids.T[:, None, :]
    scores = jnp.where(allowed, scores, NEG)
    top = jnp.max(scores, axis=2)
    weights = jnp.exp(scores - top[:, :, None])
    total = jnp.sum(weights, axis=2)
    acc = jnp.einsum("hqk,khd->qhd", to_bf16_f32(weights), v_rows.astype(jnp.float32))
    return top.T, total.T, acc


def segment_backward(q_rows, k_rows, v_rows, d_rows, lse_rows, delta_rows, row_ids, scale):
    scores = jnp.einsum("qhd,khd->hqk", q_rows.astype(jnp.float32), k_rows.astype(jnp.float32)) * scale
    allowed = row_ids.T[:, :, None] == row_ids.T[:, None, :]
    probs = jnp.exp(jnp.where(allowed, scores, NEG) - lse_rows.T[:, :, None])
    dprob = jnp.einsum("qhd,khd->hqk", d_rows.astype(jnp.float32), v_rows.astype(jnp.float32))
    dscore = to_bf16_f32(probs * (dprob - delta_rows.T[:, :, None]) * scale)
    d_q = jnp.einsum("hqk,khd->qhd", dscore, k_rows.astype(jnp.float32))
    d_k = jnp.einsum("hqk,qhd->khd", dscore, q_rows.astype(jnp.float32))
    d_v = jnp.einsum("hqk,qhd->khd", to_bf16_f32(probs), d_rows.astype(jnp.float32))
    return d_q, d_k, d_v


def reference(queries, keys, values, w_out, d_out, slide_lengths):
    head = D // H
    scale = head ** -0.5
    starts = (jnp.cumsum(slide_lengths) - slide_lengths).astype(jnp.int32)
    heads = jnp.arange(H, dtype=jnp.int32)
    ids = slide_ids(jnp.arange(TOKENS, dtype=jnp.int32), starts)
    ids = jnp.broadcast_to(ids[:, None], (TOKENS, H))
    q3 = queries.reshape(TOKENS, H, head)
    k3 = keys.reshape(TOKENS, H, head)
    v3 = values.reshape(TOKENS, H, head)
    total_bits = N_SEQ.bit_length() - 1
    dilations = [2 ** ((level * total_bits) // 3) for level in range(4)]
    top = jnp.full((TOKENS, H), NEG, jnp.float32)
    total = jnp.zeros((TOKENS, H), jnp.float32)
    acc = jnp.zeros((TOKENS, H, head), jnp.float32)
    for dilation in dilations:
        pieces = (select(q3, dilation, heads), select(k3, dilation, heads), select(v3, dilation, heads), select(ids, dilation, heads))
        level_top, level_total, level_acc = lax.map(lambda item: segment_forward(item[0], item[1], item[2], item[3], scale), pieces)
        level_top = place(level_top, dilation, heads, NEG)
        level_total = place(level_total, dilation, heads, 0.0)
        level_acc = place(level_acc, dilation, heads, 0.0)
        newer = jnp.maximum(top, level_top)
        old_factor = jnp.exp(top - newer)
        new_factor = jnp.exp(level_top - newer)
        total = total * old_factor + level_total * new_factor
        acc = acc * old_factor[..., None] + level_acc * new_factor[..., None]
        top = newer
    attended = (acc / total[..., None]).astype(jnp.bfloat16)
    lse = top + jnp.log(total)
    flat = attended.reshape(TOKENS, D)
    out = jnp.dot(flat, w_out, preferred_element_type=jnp.float32).astype(jnp.bfloat16)
    d_att = jnp.dot(d_out, w_out.T, preferred_element_type=jnp.float32).astype(jnp.bfloat16)
    d_w_out = jnp.dot(flat.T, d_out, preferred_element_type=jnp.float32) * (TOKENS ** -0.5)
    d_att3 = d_att.reshape(TOKENS, H, head)
    delta = jnp.sum(d_att3.astype(jnp.float32) * attended.astype(jnp.float32), axis=-1)
    d_q = jnp.zeros((TOKENS, H, head), jnp.float32)
    d_k = jnp.zeros((TOKENS, H, head), jnp.float32)
    d_v = jnp.zeros((TOKENS, H, head), jnp.float32)
    for dilation in dilations:
        pieces = (select(q3, dilation, heads), select(k3, dilation, heads), select(v3, dilation, heads), select(d_att3, dilation, heads), select(lse, dilation, heads), select(delta, dilation, heads), select(ids, dilation, heads))
        grads = lax.map(lambda item: segment_backward(item[0], item[1], item[2], item[3], item[4], item[5], item[6], scale), pieces)
        d_q = d_q + place(grads[0], dilation, heads, 0.0)
        d_k = d_k + place(grads[1], dilation, heads, 0.0)
        d_v = d_v + place(grads[2], dilation, heads, 0.0)
    return (out, d_q.reshape(TOKENS, D).astype(jnp.bfloat16), d_k.reshape(TOKENS, D).astype(jnp.bfloat16), d_v.reshape(TOKENS, D).astype(jnp.bfloat16), d_w_out)
```

```python
import jax
import jax.numpy as jnp
from jax import lax
from jax.experimental import pallas as pl
from jax.experimental.pallas import tpu as pltpu
from jax.sharding import PartitionSpec as P

TOKENS = 32768
HEAD = 48
ROWS = 512
WIDE = 384
HEADS = 8
NEG = -1e30
SCALE = HEAD**-0.5
LOG2E = 1.4426950408889634
C2 = SCALE * LOG2E
FAR = 1 << 30
F32 = jnp.float32
BF16 = jnp.bfloat16
MESH = pl.DeviceIdType.MESH


def nn(a, b):
    return lax.dot_general(a, b, (((1,), (0,)), ((), ())), preferred_element_type=F32)


def nt(a, b):
    return lax.dot_general(a, b, (((1,), (1,)), ((), ())), preferred_element_type=F32)


def tn(a, b):
    return lax.dot_general(a, b, (((0,), (0,)), ((), ())), preferred_element_type=F32)


def iota(shape, dim):
    return lax.broadcasted_iota(jnp.int32, shape, dim)


def token_of(a, g):
    return (a >> 7) + 4 * ((((a >> 5) & 3) + 2 * g) & 3) + 16 * ((a >> 3) & 3) + 64 * (a & 7)


def lane_head(rows):
    lane = iota((rows, WIDE), 1)
    head = jnp.zeros_like(lane)
    for i in range(1, HEADS):
        head = head + (lane >= HEAD * i).astype(jnp.int32)
    return head


def compact1(x):
    cls = lane_head(128) & 3
    y = jnp.where(cls == 0, x[0:128], x[128:256])
    y = jnp.where(cls == 2, x[256:384], y)
    return jnp.where(cls == 3, x[384:512], y)


def compact2(x1):
    return jnp.where(iota((32, WIDE), 1) < 4 * HEAD, x1[0:32], x1[32:64])


def stacked(x, n):
    rows = HEADS * n
    shift = n.bit_length() - 1
    own = (iota((rows, WIDE), 0) >> shift) == lane_head(rows)
    return jnp.where(own, jnp.concatenate([x] * HEADS, axis=0), 0.0).astype(BF16)


def to_tile(x, i):
    t, at, to = i // 4, 32 * (i % 4), 32 * (i // 4)
    tile = x[:, 128 * t : 128 * t + 128]
    shift = (to - at) % 128
    return pltpu.roll(tile, shift, 1) if shift else tile


def from_tiles(tiles):
    halves = []
    for t in range(2):
        lane = iota(tiles[0].shape, 1)
        half = None
        for i in range(4 * t, 4 * t + 4):
            at, to = 32 * (i % 4), 32 * (i // 4)
            shift = (at - to) % 128
            moved = pltpu.roll(tiles[i], shift, 1) if shift else tiles[i]
            half = moved if half is None else jnp.where((lane >> 5) == (i % 4), moved, half)
        halves.append(half)
    return jnp.concatenate(halves, axis=1)


def kernel(
    q_ref, k_ref, v_ref, w_ref, d_ref, len_ref,
    out_ref, dq_ref, dk_ref, dv_ref, dw_ref,
    p_s, pt_s, qt_s, kt_s, vt_s, dt_s, qx1, qx2, dx1, dx2,
    g1, g2, g3, kg23, vg23, kg1, vg1, p0s, p1s, p23s,
    a0, m0, lse_s, del_s, m1s, m23s, dqt, dkt, dvt,
    doth, att_s, po_send, po_recv,
    x1, x2, x3, y1, y2, y3, z1, z2, z3, r1, r2, r3,
    one_send, one_recv, s1, t1, s2, t2, s3, t3, u1, w1, u2, w2, u3, w3,
):
    seq = lax.axis_index("seq")
    g = lax.axis_index("head")
    chip = seq // 2
    core = seq % 2
    partner = {"seq": chip * 2 + (1 - core), "head": g}
    across = {"seq": seq, "head": 1 - g}

    def chip_at(c):
        return {"seq": c * 2 + core, "head": g}

    base1, base2 = (chip // 2) * 2, (chip // 8) * 8
    me1, me2, me3 = chip - base1, chip - base2, chip

    barrier = pltpu.get_barrier_semaphore()
    pl.semaphore_signal(barrier, inc=1, device_id=partner, device_id_type=MESH)
    pl.semaphore_signal(barrier, inc=1, device_id=across, device_id_type=MESH)

    @pl.loop(1, 32)
    def _(k):
        pl.semaphore_signal(barrier, inc=1, device_id=chip_at((chip + k) % 32), device_id_type=MESH)

    p_s[...] = (iota((ROWS, ROWS), 1) == token_of(iota((ROWS, ROWS), 0), g)).astype(F32).astype(BF16)
    pt_s[...] = (iota((ROWS, ROWS), 0) == token_of(iota((ROWS, ROWS), 1), g)).astype(F32).astype(BF16)

    def levels_of(x):
        y1_ = compact1(nn(p_s[...], x))
        y2_ = compact2(y1_)
        return y1_, y2_, y2_[0:8]

    ka, kb, kc = levels_of(k_ref[...])
    va, vb, vc = levels_of(v_ref[...])
    g1[core, me1, 0:128] = ka.astype(BF16)
    g1[core, me1, 128:256] = va.astype(BF16)
    g2[core, me2, 0:32] = kb.astype(BF16)
    g2[core, me2, 32:64] = vb.astype(BF16)
    g3[core, me3] = jnp.concatenate([kc, vc], axis=0).astype(BF16)

    pl.semaphore_wait(barrier, 33)

    def remote(src, dst, ss, rs, dev):
        return pltpu.make_async_remote_copy(
            src_ref=src, dst_ref=dst, send_sem=ss, recv_sem=rs, device_id=dev, device_id_type=MESH
        )

    send_d = remote(d_ref, doth, one_send.at[0], one_recv.at[0], across)
    send_d.start()

    def gather3(k):
        return remote(g3.at[core, me3], g3.at[core, me3], s3.at[k], t3.at[k], chip_at((chip + k) % 32))

    def gather2(k):
        return remote(
            g2.at[core, me2], g2.at[core, me2], s2.at[k], t2.at[k], chip_at(base2 + (me2 + k) % 8)
        )

    def gather1():
        return remote(g1.at[core, me1], g1.at[core, me1], s1.at[1], t1.at[1], chip_at(base1 + 1 - me1))

    gather1().start()

    @pl.loop(1, 8)
    def _(k):
        gather2(k).start()

    @pl.loop(1, 32)
    def _(k):
        gather3(k).start()

    qa, qb, _ = levels_of(q_ref[...])
    qx1[...] = stacked(qa, 128)
    qx2[...] = stacked(qb, 32)
    kt_s[...] = tn(k_ref[...], pt_s[...]).astype(BF16)
    qt_s[...] = tn(q_ref[...], pt_s[...]).astype(BF16)
    vt_s[...] = tn(v_ref[...], pt_s[...]).astype(BF16)

    start1 = len_ref[0]
    start2 = start1 + len_ref[1]
    start3 = start2 + len_ref[2]

    def ids_of(pos):
        return (
            (pos >= start1).astype(jnp.int32)
            + (pos >= start2).astype(jnp.int32)
            + (pos >= start3).astype(jnp.int32)
        )

    here = seq * ROWS
    id_k = ids_of(here + token_of(iota((ROWS, 1), 0), g))
    id_q = ids_of(here + token_of(iota((1, ROWS), 1), g))

    def head_rows(i):
        return pl.ds(pl.multiple_of(i * HEAD, 16), HEAD)

    @pl.loop(0, HEADS)
    def _(i):
        rows = head_rows(i)
        s = tn(kt_s[rows, :], qt_s[rows, :])
        s = jnp.where(id_k == id_q, s, NEG)
        top = jnp.max(s, axis=0, keepdims=True)
        p = jnp.exp2((s - top) * C2)
        total = jnp.sum(p, axis=0, keepdims=True)
        m0[pl.ds(i, 1), :] = top
        lse_s[pl.ds(i, 1), :] = top * C2 + jnp.log2(total)
        pb = p.astype(BF16)
        p0s[i] = pb
        a0[rows, :] = nn(vt_s[rows, :], pb) / total

    @pl.loop(1, 32)
    def _(k):
        gather3(k).wait()

    core3 = remote(g3.at[core], g3.at[core], s3.at[0], t3.at[0], partner)
    core3.start()

    @pl.loop(1, 8)
    def _(k):
        gather2(k).wait()

    core2 = remote(g2.at[core], g2.at[core], s2.at[0], t2.at[0], partner)
    core2.start()
    gather1().wait()
    core1 = remote(g1.at[core], g1.at[core], s1.at[0], t1.at[0], partner)
    core1.start()

    def slide_range(pos):
        lo = jnp.where(pos >= start1, start1, 0)
        lo = jnp.where(pos >= start2, start2, lo)
        lo = jnp.where(pos >= start3, start3, lo)
        hi = jnp.where(pos < start3, start3, TOKENS)
        hi = jnp.where(pos < start2, start2, hi)
        hi = jnp.where(pos < start1, start1, hi)
        return lo, hi

    def masked(s, key_pos, lo, hi):
        return jnp.where((key_pos >= lo) & (key_pos < hi), s, NEG)

    core3.wait()
    core2.wait()
    three = g3[...].astype(F32).reshape(64, 16, WIDE)
    kg23[0:512] = g2[:, :, 0:32].reshape(512, WIDE)
    vg23[0:512] = g2[:, :, 32:64].reshape(512, WIDE)
    kg23[512:1024] = three[:, 0:8].reshape(512, WIDE).astype(BF16)
    vg23[512:1024] = three[:, 8:16].reshape(512, WIDE).astype(BF16)

    row = iota((512, 1), 0)
    col = iota((1, 256), 1)
    inner = col & 31
    off = 8 * g + (col >> 5)
    lo, hi = slide_range(here + off + 16 * (inner >> 3) + 64 * (inner & 7))
    lo, hi = lo - off, hi - off
    pos2 = 512 * (2 * (base2 + ((row >> 5) & 7)) + (row >> 8)) + 16 * ((row >> 3) & 3) + 64 * (row & 7)
    pos3 = 512 * (2 * ((row >> 3) & 31) + (row >> 8)) + 64 * (row & 7)
    sa = masked(nt(kg23[0:512], qx2[...]), pos2, lo, hi)
    sb = masked(nt(kg23[512:1024], qx2[...]), pos3, jnp.where(inner < 8, lo, FAR), hi)
    top23 = jnp.maximum(jnp.max(sa, axis=0, keepdims=True), jnp.max(sb, axis=0, keepdims=True))
    pa = jnp.exp2((sa - top23) * C2)
    pb3 = jnp.exp2((sb - top23) * C2)
    sum23 = jnp.sum(pa, axis=0, keepdims=True) + jnp.sum(pb3, axis=0, keepdims=True)
    p23s[0:512] = pa.astype(BF16)
    p23s[512:1024] = pb3.astype(BF16)
    m23s[...] = jnp.broadcast_to(top23, (8, 256))
    acc23 = tn(vg23[...], p23s[...])

    core1.wait()
    kg1[...] = g1[:, :, 0:128].reshape(512, WIDE)
    vg1[...] = g1[:, :, 128:256].reshape(512, WIDE)
    colb = iota((1, 1024), 1)
    offb = (colb >> 7) & 3

    def spread1(j):
        return 4 * ((((j >> 5) & 3) + 2 * g) & 3) + 16 * ((j >> 3) & 3) + 64 * (j & 7)

    lo1, hi1 = slide_range(here + offb + spread1(colb & 127))
    lo1, hi1 = lo1 - offb, hi1 - offb
    pos1 = 512 * (2 * (base1 + ((row >> 7) & 1)) + (row >> 8)) + spread1(row & 127)
    sc = masked(nt(kg1[...], qx1[...]), pos1, lo1, hi1)
    top1 = jnp.max(sc, axis=0, keepdims=True)
    pc = jnp.exp2((sc - top1) * C2)
    sum1 = jnp.sum(pc, axis=0, keepdims=True)
    p1s[...] = pc.astype(BF16)
    m1s[...] = jnp.broadcast_to(top1, (8, 1024))
    acc1 = tn(vg1[...], p1s[...])

    st23 = jnp.broadcast_to(top23, (8, 256))
    su23 = jnp.broadcast_to(sum23, (8, 256))
    lane8 = iota((8, 128), 1) >> 5
    lane48 = iota((HEAD, 128), 1) >> 5
    for i in range(HEADS):
        r = slice(HEAD * i, HEAD * i + HEAD)
        c = slice(128 * (i % 4), 128 * (i % 4) + 128)
        t = slice(128 * i, 128 * i + 128)
        two = jnp.where(lane8 == i // 4, to_tile(st23, i), NEG)[0:1]
        two_sum = jnp.where(lane8 == i // 4, to_tile(su23, i), 0.0)[0:1]
        two_acc = jnp.where(lane48 == i // 4, to_tile(acc23[r], i), 0.0)
        zero = lse_s[i : i + 1, c]
        one = top1[:, t] * C2
        two = two * C2
        new = jnp.maximum(jnp.maximum(zero, one), two)
        f0 = jnp.exp2(zero - new)
        f1 = jnp.exp2(one - new)
        f2 = jnp.exp2(two - new)
        l_new = f0 + sum1[:, t] * f1 + two_sum * f2
        a_new = (a0[r, c] * f0 + acc1[r, t] * f1 + two_acc * f2) / l_new
        a0[r, c] = a_new
        lse_s[i : i + 1, c] = new + jnp.log2(l_new)

    att_t = a0[...].astype(BF16)
    att = nt(pt_s[...], att_t).astype(BF16)
    att_s[...] = att
    own = pl.ds(pl.multiple_of(g * WIDE, 128), WIDE)
    other = pl.ds(pl.multiple_of((1 - g) * WIDE, 128), WIDE)
    po_send[...] = nn(att, w_ref[:, other]).astype(BF16)
    send_o = remote(po_send, po_recv, one_send.at[1], one_recv.at[1], across)
    send_o.start()

    send_d.wait()
    d_att = (nt(d_ref[...], w_ref[:, own]) + nt(doth[...], w_ref[:, other])).astype(BF16)
    dt = tn(d_att, pt_s[...])
    dt_s[...] = dt.astype(BF16)
    da, db, _ = levels_of(d_att)
    dx1[...] = stacked(da, 128)
    dx2[...] = stacked(db, 32)
    prod = dt * att_t.astype(F32)
    for i in range(HEADS):
        del_s[i : i + 1, :] = jnp.sum(prod[HEAD * i : HEAD * i + HEAD], axis=0, keepdims=True)

    srow = iota((512, WIDE), 0)
    u = srow & 15
    source = 12 * (2 * ((srow >> 4) & 15) + (srow >> 8)) + u
    sel = ((iota((512, WIDE), 1) == source) & (u < 12)).astype(F32).astype(BF16)
    for part, block in ((g, d_ref), (1 - g, doth)):
        term = nn(sel, tn(block[...], att).astype(BF16)).astype(BF16).reshape(2, 16, 16, WIDE)
        x3[:, pl.ds(16 * part, 16), 16:32] = term

    def tiles_of(ref):
        return [
            jnp.broadcast_to(ref[i : i + 1, 128 * (i % 4) : 128 * (i % 4) + 128], (8, 128))
            for i in range(HEADS)
        ]

    lse_tiles, del_tiles = tiles_of(lse_s), tiles_of(del_s)
    lse23 = from_tiles(lse_tiles)[0:1]
    del23 = from_tiles(del_tiles)[0:1]
    p = p23s[...].astype(F32) * jnp.exp2(m23s[0:1] * C2 - lse23)
    ds = (p * (nt(vg23[...], dx2[...]) - del23)).astype(BF16)
    dk23 = nn(ds, qx2[...])
    dv23 = nn(p.astype(BF16), dx2[...])
    dq23 = tn(kg23[...], ds)
    x2[:, :, 0:32] = dk23[0:512].reshape(2, 8, 32, WIDE).astype(BF16)
    x2[:, :, 32:64] = dv23[0:512].reshape(2, 8, 32, WIDE).astype(BF16)
    x3[:, :, 0:16] = jnp.concatenate(
        [dk23[512:1024].reshape(2, 32, 8, WIDE), dv23[512:1024].reshape(2, 32, 8, WIDE)], axis=2
    ).astype(BF16)
    swap3 = remote(x3.at[1 - core], y3, u3.at[0], w3.at[0], partner)
    swap3.start()
    swap2 = remote(x2.at[1 - core], y2, u2.at[0], w2.at[0], partner)
    swap2.start()

    lse1 = jnp.concatenate([t[0:1] for t in lse_tiles], axis=1)
    del1 = jnp.concatenate([t[0:1] for t in del_tiles], axis=1)
    p = p1s[...].astype(F32) * jnp.exp2(m1s[0:1] * C2 - lse1)
    ds = (p * (nt(vg1[...], dx1[...]) - del1)).astype(BF16)
    dk1 = nn(ds, qx1[...])
    dv1 = nn(p.astype(BF16), dx1[...])
    dq1 = tn(kg1[...], ds)
    x1[:, :, 0:128] = dk1.reshape(2, 2, 128, WIDE).astype(BF16)
    x1[:, :, 128:256] = dv1.reshape(2, 2, 128, WIDE).astype(BF16)
    swap1 = remote(x1.at[1 - core], y1, u1.at[0], w1.at[0], partner)
    swap1.start()

    swap3.wait()
    z3[...] = (x3[core].astype(F32) + y3[...].astype(F32)).astype(BF16)
    swap2.wait()
    z2[...] = (x2[core].astype(F32) + y2[...].astype(F32)).astype(BF16)
    r3[me3] = z3[me3]
    r2[me2] = z2[me2]
    swap1.wait()
    z1[...] = (x1[core].astype(F32) + y1[...].astype(F32)).astype(BF16)
    r1[me1] = z1[me1]

    def reduce3(k):
        to = (chip + k) % 32
        return remote(z3.at[to], r3.at[me3], u3.at[k], w3.at[k], chip_at(to))

    def reduce2(k):
        to = (me2 + k) % 8
        return remote(z2.at[to], r2.at[me2], u2.at[k], w2.at[k], chip_at(base2 + to))

    def reduce1():
        return remote(z1.at[1 - me1], r1.at[me1], u1.at[1], w1.at[1], chip_at(base1 + 1 - me1))

    @pl.loop(1, 32)
    def _(k):
        reduce3(k).start()

    @pl.loop(1, 8)
    def _(k):
        reduce2(k).start()

    reduce1().start()

    a0[...] = jnp.concatenate(
        [jnp.exp2(m0[...] * C2 - lse_s[...])] * (WIDE // HEADS), axis=0
    )

    @pl.loop(0, HEADS)
    def _(i):
        rows = head_rows(i)
        p = p0s[i].astype(F32) * a0[pl.ds(i, 1), :]
        pb = p.astype(BF16)
        dp = tn(vt_s[rows, :], dt_s[rows, :])
        ds = (p * (dp - del_s[pl.ds(i, 1), :])).astype(BF16)
        dqt[rows, :] = nn(kt_s[rows, :], ds)
        dkt[rows, :] = nt(qt_s[rows, :], ds)
        dvt[rows, :] = nt(dt_s[rows, :], pb)

    for i in range(HEADS):
        r = slice(HEAD * i, HEAD * i + HEAD)
        c = slice(128 * (i % 4), 128 * (i % 4) + 128)
        t = slice(128 * i, 128 * i + 128)
        two = jnp.where(lane48 == i // 4, to_tile(dq23[r], i), 0.0)
        dqt[r, c] = dqt[r, c] + dq1[r, t] + two
    dq_ref[...] = nt(pt_s[...], (dqt[...] * SCALE).astype(BF16)).astype(BF16)

    send_o.wait()
    out_ref[...] = (nn(att_s[...], w_ref[:, own]) + po_recv[...].astype(F32)).astype(BF16)

    @pl.loop(1, 32)
    def _(k):
        reduce3(k).wait()

    @pl.loop(1, 8)
    def _(k):
        reduce2(k).wait()

    reduce1().wait()
    three = jnp.sum(r3[...].astype(F32), axis=0)
    two = jnp.sum(r2[...].astype(F32), axis=0)
    one = jnp.sum(r1[...].astype(F32), axis=0)
    dw_ref[...] = three[16:32] * (TOKENS**-0.5)
    low = iota((32, WIDE), 1) < 4 * HEAD
    cls = lane_head(128) & 3

    def whole(first, second, third, level0, scale):
        second = jnp.concatenate([second[0:8] + third, second[8:32]], axis=0)
        first = jnp.concatenate(
            [
                first[0:32] + jnp.where(low, second, 0.0),
                first[32:64] + jnp.where(low, 0.0, second),
                first[64:128],
            ],
            axis=0,
        )
        first = first * scale
        full = jnp.concatenate([jnp.where(cls == j, first, 0.0) for j in range(4)], axis=0)
        total = nn(pt_s[...], full.astype(BF16)) + nt(pt_s[...], (level0 * scale).astype(BF16))
        return total.astype(BF16)

    dk_ref[...] = whole(one[0:128], two[0:32], three[0:8], dkt[...], SCALE)
    dv_ref[...] = whole(one[128:256], two[32:64], three[8:16], dvt[...], 1.0)


def shards(queries, keys, values, w_out, d_out, slide_lengths):
    vmem = pl.BlockSpec(memory_space=pltpu.VMEM)
    shape = jax.ShapeDtypeStruct

    def v(*dims, dtype=BF16):
        return pltpu.VMEM(dims, dtype)

    def sems(n):
        return pltpu.SemaphoreType.DMA((n,))

    scratch = [
        v(512, 512), v(512, 512),
        v(WIDE, 512), v(WIDE, 512), v(WIDE, 512), v(WIDE, 512),
        v(1024, WIDE), v(256, WIDE), v(1024, WIDE), v(256, WIDE),
        v(2, 2, 256, WIDE), v(2, 8, 64, WIDE), v(2, 32, 16, WIDE),
        v(1024, WIDE), v(1024, WIDE), v(512, WIDE), v(512, WIDE),
        v(8, 512, 512), v(512, 1024), v(1024, 256),
        v(WIDE, 512, dtype=F32), v(8, 512, dtype=F32),
        v(8, 512, dtype=F32), v(8, 512, dtype=F32), v(8, 1024, dtype=F32), v(8, 256, dtype=F32),
        v(WIDE, 512, dtype=F32), v(WIDE, 512, dtype=F32), v(WIDE, 512, dtype=F32),
        v(512, WIDE), v(512, WIDE), v(512, WIDE), v(512, WIDE),
        v(2, 2, 256, WIDE), v(2, 8, 64, WIDE), v(2, 32, 32, WIDE),
        v(2, 256, WIDE), v(8, 64, WIDE), v(32, 32, WIDE),
        v(2, 256, WIDE), v(8, 64, WIDE), v(32, 32, WIDE),
        v(2, 256, WIDE), v(8, 64, WIDE), v(32, 32, WIDE),
        sems(2), sems(2),
        sems(2), sems(2), sems(8), sems(8), sems(32), sems(32),
        sems(2), sems(2), sems(8), sems(8), sems(32), sems(32),
    ]
    out, dq, dk, dv, dw = pl.pallas_call(
        kernel,
        out_shape=[shape((ROWS, WIDE), BF16)] * 4 + [shape((16, WIDE), F32)],
        in_specs=[vmem] * 5 + [pl.BlockSpec(memory_space=pltpu.SMEM)],
        out_specs=[vmem] * 5,
        scratch_shapes=scratch,
        compiler_params=pltpu.CompilerParams(
            collective_id=0, has_side_effects=True, vmem_limit_bytes=60 * 1024 * 1024
        ),
    )(queries, keys, values, w_out, d_out, slide_lengths)
    return out, dq, dk, dv, dw[:12].T


def solution(mesh):
    both = P("seq", "head")
    return jax.shard_map(
        shards,
        mesh=mesh,
        in_specs=(both, both, both, P("head", None), both, P()),
        out_specs=(both, both, both, both, P("head", "seq")),
        check_vma=False,
    )
```

```python
import jax
import jax.numpy as jnp
from jax import lax
from jax.experimental import pallas as pl
from jax.experimental.pallas import tpu as pltpu
from jax.sharding import PartitionSpec as P

TOKENS = 32768
HEAD = 48
ROWS = 512
WIDE = 384
HEADS = 8
NEG = -1e30
SCALE = HEAD**-0.5
LOG2E = 1.4426950408889634
C2 = SCALE * LOG2E
FAR = 1 << 30
F32 = jnp.float32
BF16 = jnp.bfloat16
MESH = pl.DeviceIdType.MESH


def nn(a, b):
    return lax.dot_general(a, b, (((1,), (0,)), ((), ())), preferred_element_type=F32)


def nt(a, b):
    return lax.dot_general(a, b, (((1,), (1,)), ((), ())), preferred_element_type=F32)


def tn(a, b):
    return lax.dot_general(a, b, (((0,), (0,)), ((), ())), preferred_element_type=F32)


def iota(shape, dim):
    return lax.broadcasted_iota(jnp.int32, shape, dim)


def token_of(a, g):
    return (a >> 7) + 4 * ((((a >> 5) & 3) + 2 * g) & 3) + 16 * ((a >> 3) & 3) + 64 * (a & 7)


def lane_head(rows):
    lane = iota((rows, WIDE), 1)
    head = jnp.zeros_like(lane)
    for i in range(1, HEADS):
        head = head + (lane >= HEAD * i).astype(jnp.int32)
    return head


def compact1(x):
    cls = lane_head(128) & 3
    y = jnp.where(cls == 0, x[0:128], x[128:256])
    y = jnp.where(cls == 2, x[256:384], y)
    return jnp.where(cls == 3, x[384:512], y)


def compact2(x1):
    return jnp.where(iota((32, WIDE), 1) < 4 * HEAD, x1[0:32], x1[32:64])


def stacked(x, n):
    rows = HEADS * n
    shift = n.bit_length() - 1
    own = (iota((rows, WIDE), 0) >> shift) == lane_head(rows)
    return jnp.where(own, jnp.concatenate([x] * HEADS, axis=0), 0.0).astype(BF16)


def to_tile(x, i):
    t, at, to = i // 4, 32 * (i % 4), 32 * (i // 4)
    tile = x[:, 128 * t : 128 * t + 128]
    shift = (to - at) % 128
    return pltpu.roll(tile, shift, 1) if shift else tile


def from_tiles(tiles):
    halves = []
    for t in range(2):
        lane = iota(tiles[0].shape, 1)
        half = None
        for i in range(4 * t, 4 * t + 4):
            at, to = 32 * (i % 4), 32 * (i // 4)
            shift = (at - to) % 128
            moved = pltpu.roll(tiles[i], shift, 1) if shift else tiles[i]
            half = moved if half is None else jnp.where((lane >> 5) == (i % 4), moved, half)
        halves.append(half)
    return jnp.concatenate(halves, axis=1)


def kernel(
    q_in, k_in, v_in, w_in, d_in, len_in,
    out_ref, dq_ref, dk_ref, dv_ref, dw_ref,
    q_ref, k_ref, v_ref, w_ref, d_ref, len_ref, in_sem,
    p_s, pt_s, qt_s, kt_s, vt_s, dt_s, qx1, qx2, dx1, dx2,
    g1, g2, g3, kg23, vg23, kg1, vg1, p0s, p1s, p23s,
    a0, m0, lse_s, del_s, m1s, m23s, dqt, dkt, dvt, base_k, base_v,
    doth, att_s, po_send, po_recv,
    x1, x2, x3, x4, y1, y2, y3, y4, z1, z2, z3, z4, r1, r2, r3, r4,
    one_send, one_recv, s1, t1, s2, t2, s3, t3, u1, w1, u2, w2, u3, w3, u4, w4,
):
    seq = lax.axis_index("seq")
    g = lax.axis_index("head")
    chip = seq // 2
    core = seq % 2
    partner = {"seq": chip * 2 + (1 - core), "head": g}
    across = {"seq": seq, "head": 1 - g}

    def chip_at(c):
        return {"seq": c * 2 + core, "head": g}

    base1, base2 = (chip // 2) * 2, (chip // 8) * 8
    me1, me2, me3 = chip - base1, chip - base2, chip

    loads = [
        pltpu.make_async_copy(a, b, in_sem.at[n])
        for n, (a, b) in enumerate(
            ((k_in, k_ref), (v_in, v_ref), (q_in, q_ref), (d_in, d_ref), (w_in, w_ref), (len_in, len_ref))
        )
    ]
    for load in loads:
        load.start()
    barrier = pltpu.get_barrier_semaphore()
    pl.semaphore_signal(barrier, inc=1, device_id=partner, device_id_type=MESH)
    pl.semaphore_signal(barrier, inc=1, device_id=across, device_id_type=MESH)

    @pl.loop(1, 32)
    def _(k):
        pl.semaphore_signal(barrier, inc=1, device_id=chip_at((chip + k) % 32), device_id_type=MESH)

    p_s[...] = (iota((ROWS, ROWS), 1) == token_of(iota((ROWS, ROWS), 0), g)).astype(F32).astype(BF16)
    pt_s[...] = (iota((ROWS, ROWS), 0) == token_of(iota((ROWS, ROWS), 1), g)).astype(F32).astype(BF16)

    def levels_of(x):
        y1_ = compact1(nn(p_s[...], x))
        y2_ = compact2(y1_)
        return y1_, y2_, y2_[0:8]

    loads[0].wait()
    ka, kb, kc = levels_of(k_ref[...])
    loads[1].wait()
    va, vb, vc = levels_of(v_ref[...])
    g1[core, me1, 0:128] = ka.astype(BF16)
    g1[core, me1, 128:256] = va.astype(BF16)
    g2[core, me2, 0:32] = kb.astype(BF16)
    g2[core, me2, 32:64] = vb.astype(BF16)
    g3[core, me3] = jnp.concatenate([kc, vc], axis=0).astype(BF16)

    pl.semaphore_wait(barrier, 33)

    def remote(src, dst, ss, rs, dev):
        return pltpu.make_async_remote_copy(
            src_ref=src, dst_ref=dst, send_sem=ss, recv_sem=rs, device_id=dev, device_id_type=MESH
        )

    def gather3(k):
        return remote(g3.at[core, me3], g3.at[core, me3], s3.at[k], t3.at[k], chip_at((chip + k) % 32))

    def gather2(k):
        return remote(
            g2.at[core, me2], g2.at[core, me2], s2.at[k], t2.at[k], chip_at(base2 + (me2 + k) % 8)
        )

    def gather1():
        return remote(g1.at[core, me1], g1.at[core, me1], s1.at[1], t1.at[1], chip_at(base1 + 1 - me1))

    @pl.loop(1, 32)
    def _(k):
        gather3(k).start()

    @pl.loop(1, 8)
    def _(k):
        gather2(k).start()

    gather1().start()

    loads[3].wait()
    send_d = remote(d_ref, doth, one_send.at[0], one_recv.at[0], across)
    send_d.start()

    loads[2].wait()
    qa, qb, _ = levels_of(q_ref[...])
    qx1[...] = stacked(qa, 128)
    qx2[...] = stacked(qb, 32)
    kt_s[...] = tn(k_ref[...], pt_s[...]).astype(BF16)
    qt_s[...] = tn(q_ref[...], pt_s[...]).astype(BF16)
    vt_s[...] = tn(v_ref[...], pt_s[...]).astype(BF16)

    loads[5].wait()
    start1 = len_ref[0]
    start2 = start1 + len_ref[1]
    start3 = start2 + len_ref[2]

    def ids_of(pos):
        return (
            (pos >= start1).astype(jnp.int32)
            + (pos >= start2).astype(jnp.int32)
            + (pos >= start3).astype(jnp.int32)
        )

    here = seq * ROWS
    id_k = ids_of(here + token_of(iota((ROWS, 1), 0), g))
    id_q = ids_of(here + token_of(iota((1, ROWS), 1), g))

    def head_rows(i):
        return pl.ds(pl.multiple_of(i * HEAD, 16), HEAD)

    @pl.loop(0, HEADS)
    def _(i):
        rows = head_rows(i)
        s = tn(kt_s[rows, :], qt_s[rows, :])
        s = jnp.where(id_k == id_q, s, NEG)
        top = jnp.max(s, axis=0, keepdims=True)
        p = jnp.exp2((s - top) * C2)
        total = jnp.sum(p, axis=0, keepdims=True)
        m0[pl.ds(i, 1), :] = top
        lse_s[pl.ds(i, 1), :] = top * C2 + jnp.log2(total)
        pb = p.astype(BF16)
        p0s[i] = pb
        a0[rows, :] = nn(vt_s[rows, :], pb) / total

    @pl.loop(1, 32)
    def _(k):
        gather3(k).wait()

    core3 = remote(g3.at[core], g3.at[core], s3.at[0], t3.at[0], partner)
    core3.start()

    @pl.loop(1, 8)
    def _(k):
        gather2(k).wait()

    core2 = remote(g2.at[core], g2.at[core], s2.at[0], t2.at[0], partner)
    core2.start()
    gather1().wait()
    core1 = remote(g1.at[core], g1.at[core], s1.at[0], t1.at[0], partner)
    core1.start()

    loads[4].wait()
    own = pl.ds(pl.multiple_of(g * WIDE, 128), WIDE)
    other = pl.ds(pl.multiple_of((1 - g) * WIDE, 128), WIDE)
    send_d.wait()
    d_att = (nt(d_ref[...], w_ref[:, own]) + nt(doth[...], w_ref[:, other])).astype(BF16)
    dt = tn(d_att, pt_s[...])
    dt_s[...] = dt.astype(BF16)
    da, db, _ = levels_of(d_att)
    dx1[...] = stacked(da, 128)
    dx2[...] = stacked(db, 32)

    def slide_range(pos):
        lo = jnp.where(pos >= start1, start1, 0)
        lo = jnp.where(pos >= start2, start2, lo)
        lo = jnp.where(pos >= start3, start3, lo)
        hi = jnp.where(pos < start3, start3, TOKENS)
        hi = jnp.where(pos < start2, start2, hi)
        hi = jnp.where(pos < start1, start1, hi)
        return lo, hi

    def masked(s, key_pos, lo, hi):
        return jnp.where((key_pos >= lo) & (key_pos < hi), s, NEG)

    core3.wait()
    core2.wait()
    three = g3[...].astype(F32).reshape(64, 16, WIDE)
    kg23[0:512] = g2[:, :, 0:32].reshape(512, WIDE)
    vg23[0:512] = g2[:, :, 32:64].reshape(512, WIDE)
    kg23[512:1024] = three[:, 0:8].reshape(512, WIDE).astype(BF16)
    vg23[512:1024] = three[:, 8:16].reshape(512, WIDE).astype(BF16)

    row = iota((512, 1), 0)
    col = iota((1, 256), 1)
    inner = col & 31
    off = 8 * g + (col >> 5)
    lo, hi = slide_range(here + off + 16 * (inner >> 3) + 64 * (inner & 7))
    lo, hi = lo - off, hi - off
    pos2 = 512 * (2 * (base2 + ((row >> 5) & 7)) + (row >> 8)) + 16 * ((row >> 3) & 3) + 64 * (row & 7)
    pos3 = 512 * (2 * ((row >> 3) & 31) + (row >> 8)) + 64 * (row & 7)
    sa = masked(nt(kg23[0:512], qx2[...]), pos2, lo, hi)
    sb = masked(nt(kg23[512:1024], qx2[...]), pos3, jnp.where(inner < 8, lo, FAR), hi)
    top23 = jnp.maximum(jnp.max(sa, axis=0, keepdims=True), jnp.max(sb, axis=0, keepdims=True))
    pa = jnp.exp2((sa - top23) * C2)
    pb3 = jnp.exp2((sb - top23) * C2)
    sum23 = jnp.sum(pa, axis=0, keepdims=True) + jnp.sum(pb3, axis=0, keepdims=True)
    p23s[0:512] = pa.astype(BF16)
    p23s[512:1024] = pb3.astype(BF16)
    m23s[...] = jnp.broadcast_to(top23, (8, 256))
    acc23 = tn(vg23[...], p23s[...])

    core1.wait()
    kg1[...] = g1[:, :, 0:128].reshape(512, WIDE)
    vg1[...] = g1[:, :, 128:256].reshape(512, WIDE)
    colb = iota((1, 1024), 1)
    offb = (colb >> 7) & 3

    def spread1(j):
        return 4 * ((((j >> 5) & 3) + 2 * g) & 3) + 16 * ((j >> 3) & 3) + 64 * (j & 7)

    lo1, hi1 = slide_range(here + offb + spread1(colb & 127))
    lo1, hi1 = lo1 - offb, hi1 - offb
    pos1 = 512 * (2 * (base1 + ((row >> 7) & 1)) + (row >> 8)) + spread1(row & 127)
    top1, sum1, acc1 = [], [], []
    for half in range(2):
        c = slice(512 * half, 512 * half + 512)
        w = slice(128 * half, 128 * half + 256)
        sc = masked(nt(kg1[:, w], qx1[c, w]), pos1, lo1[:, c], hi1[:, c])
        top1.append(jnp.max(sc, axis=0, keepdims=True))
        pc = jnp.exp2((sc - top1[half]) * C2)
        sum1.append(jnp.sum(pc, axis=0, keepdims=True))
        p1s[:, c] = pc.astype(BF16)
        m1s[:, c] = jnp.broadcast_to(top1[half], (8, 512))
        acc1.append(tn(vg1[:, w], p1s[:, c]))

    st23 = jnp.broadcast_to(top23, (8, 256))
    su23 = jnp.broadcast_to(sum23, (8, 256))
    lane8 = iota((8, 128), 1) >> 5
    lane48 = iota((HEAD, 128), 1) >> 5
    for i in range(HEADS):
        r = slice(HEAD * i, HEAD * i + HEAD)
        c = slice(128 * (i % 4), 128 * (i % 4) + 128)
        half = i // 4
        rr = slice(HEAD * i - 128 * half, HEAD * i - 128 * half + HEAD)
        two = jnp.where(lane8 == i // 4, to_tile(st23, i), NEG)[0:1]
        two_sum = jnp.where(lane8 == i // 4, to_tile(su23, i), 0.0)[0:1]
        two_acc = jnp.where(lane48 == i // 4, to_tile(acc23[r], i), 0.0)
        zero = lse_s[i : i + 1, c]
        one = top1[half][:, c] * C2
        two = two * C2
        new = jnp.maximum(jnp.maximum(zero, one), two)
        f0 = jnp.exp2(zero - new)
        f1 = jnp.exp2(one - new)
        f2 = jnp.exp2(two - new)
        l_new = f0 + sum1[half][:, c] * f1 + two_sum * f2
        a_new = (a0[r, c] * f0 + acc1[half][rr, c] * f1 + two_acc * f2) / l_new
        a0[r, c] = a_new
        lse_s[i : i + 1, c] = new + jnp.log2(l_new)

    att_t = a0[...].astype(BF16)
    att = nt(pt_s[...], att_t).astype(BF16)
    att_s[...] = att
    po_send[...] = nn(att, w_ref[:, other]).astype(BF16)
    send_o = remote(po_send, po_recv, one_send.at[1], one_recv.at[1], across)
    send_o.start()

    for part, block in ((g, d_ref), (1 - g, doth)):
        term = tn(block[...], att)
        for c in range(16):
            x4[0, 16 * part + c] = term[24 * c : 24 * c + 16].astype(BF16)
            x4[1, 16 * part + c] = term[24 * c + 8 : 24 * c + 24].astype(BF16)
    swap4 = remote(x4.at[1 - core], y4, u4.at[0], w4.at[0], partner)
    swap4.start()
    prod = dt_s[...].astype(F32) * att_t.astype(F32)
    for i in range(HEADS):
        del_s[i : i + 1, :] = jnp.sum(prod[HEAD * i : HEAD * i + HEAD], axis=0, keepdims=True)

    swap4.wait()
    z4[...] = (x4[core].astype(F32) + y4[...].astype(F32)).astype(BF16)
    r4[me3] = z4[me3]

    def reduce4(k):
        to = (chip + k) % 32
        return remote(z4.at[to], r4.at[me3], u4.at[k], w4.at[k], chip_at(to))

    @pl.loop(1, 32)
    def _(k):
        reduce4(k).start()

    def tiles_of(ref):
        return [
            jnp.broadcast_to(ref[i : i + 1, 128 * (i % 4) : 128 * (i % 4) + 128], (8, 128))
            for i in range(HEADS)
        ]

    lse_tiles, del_tiles = tiles_of(lse_s), tiles_of(del_s)
    lse23 = from_tiles(lse_tiles)[0:1]
    del23 = from_tiles(del_tiles)[0:1]
    p = p23s[...].astype(F32) * jnp.exp2(m23s[0:1] * C2 - lse23)
    ds = (p * (nt(vg23[...], dx2[...]) - del23)).astype(BF16)
    dk23 = nn(ds, qx2[...])
    dv23 = nn(p.astype(BF16), dx2[...])
    dq23 = tn(kg23[...], ds)
    x2[:, :, 0:32] = dk23[0:512].reshape(2, 8, 32, WIDE).astype(BF16)
    x2[:, :, 32:64] = dv23[0:512].reshape(2, 8, 32, WIDE).astype(BF16)
    x3[...] = jnp.concatenate(
        [dk23[512:1024].reshape(2, 32, 8, WIDE), dv23[512:1024].reshape(2, 32, 8, WIDE)], axis=2
    ).astype(BF16)
    swap3 = remote(x3.at[1 - core], y3, u3.at[0], w3.at[0], partner)
    swap3.start()
    swap2 = remote(x2.at[1 - core], y2, u2.at[0], w2.at[0], partner)
    swap2.start()

    lse1 = jnp.concatenate([t[0:1] for t in lse_tiles], axis=1)
    del1 = jnp.concatenate([t[0:1] for t in del_tiles], axis=1)
    dk1, dv1, dq1 = [], [], []
    for half in range(2):
        c = slice(512 * half, 512 * half + 512)
        w = slice(128 * half, 128 * half + 256)
        p = p1s[:, c].astype(F32) * jnp.exp2(m1s[0:1, c] * C2 - lse1[:, c])
        ds = (p * (nt(vg1[:, w], dx1[c, w]) - del1[:, c])).astype(BF16)
        dk1.append(nn(ds, qx1[c, w]))
        dv1.append(nn(p.astype(BF16), dx1[c, w]))
        dq1.append(tn(kg1[:, w], ds))

    def joined(a, b):
        return jnp.concatenate([a[:, 0:128], a[:, 128:256] + b[:, 0:128], b[:, 128:256]], axis=1)

    dk1, dv1 = joined(*dk1), joined(*dv1)
    x1[:, :, 0:128] = dk1.reshape(2, 2, 128, WIDE).astype(BF16)
    x1[:, :, 128:256] = dv1.reshape(2, 2, 128, WIDE).astype(BF16)
    swap1 = remote(x1.at[1 - core], y1, u1.at[0], w1.at[0], partner)
    swap1.start()

    swap3.wait()
    z3[...] = (x3[core].astype(F32) + y3[...].astype(F32)).astype(BF16)
    swap2.wait()
    z2[...] = (x2[core].astype(F32) + y2[...].astype(F32)).astype(BF16)
    r3[me3] = z3[me3]
    r2[me2] = z2[me2]
    swap1.wait()
    z1[...] = (x1[core].astype(F32) + y1[...].astype(F32)).astype(BF16)
    r1[me1] = z1[me1]

    def reduce3(k):
        to = (chip + k) % 32
        return remote(z3.at[to], r3.at[me3], u3.at[k], w3.at[k], chip_at(to))

    def reduce2(k):
        to = (me2 + k) % 8
        return remote(z2.at[to], r2.at[me2], u2.at[k], w2.at[k], chip_at(base2 + to))

    def reduce1():
        return remote(z1.at[1 - me1], r1.at[me1], u1.at[1], w1.at[1], chip_at(base1 + 1 - me1))

    @pl.loop(1, 32)
    def _(k):
        reduce3(k).start()

    @pl.loop(1, 8)
    def _(k):
        reduce2(k).start()

    reduce1().start()

    a0[...] = jnp.concatenate(
        [jnp.exp2(m0[...] * C2 - lse_s[...])] * (WIDE // HEADS), axis=0
    )

    @pl.loop(0, HEADS)
    def _(i):
        rows = head_rows(i)
        p = p0s[i].astype(F32) * a0[pl.ds(i, 1), :]
        pb = p.astype(BF16)
        dp = tn(vt_s[rows, :], dt_s[rows, :])
        ds = (p * (dp - del_s[pl.ds(i, 1), :])).astype(BF16)
        dqt[rows, :] = nn(kt_s[rows, :], ds)
        dkt[rows, :] = nt(qt_s[rows, :], ds)
        dvt[rows, :] = nt(dt_s[rows, :], pb)

    for i in range(HEADS):
        r = slice(HEAD * i, HEAD * i + HEAD)
        c = slice(128 * (i % 4), 128 * (i % 4) + 128)
        half = i // 4
        rr = slice(HEAD * i - 128 * half, HEAD * i - 128 * half + HEAD)
        two = jnp.where(lane48 == half, to_tile(dq23[r], i), 0.0)
        dqt[r, c] = dqt[r, c] + dq1[half][rr, c] + two
    dq_ref[...] = nt(pt_s[...], (dqt[...] * SCALE).astype(BF16)).astype(BF16)

    for level0, scale, kept in ((dkt, SCALE, base_k), (dvt, 1.0, base_v)):
        kept[...] = nt(pt_s[...], (level0[...] * scale).astype(BF16))

    send_o.wait()
    out_ref[...] = (nn(att_s[...], w_ref[:, own]) + po_recv[...].astype(F32)).astype(BF16)

    @pl.loop(1, 32)
    def _(k):
        reduce3(k).wait()
        reduce4(k).wait()

    @pl.loop(1, 8)
    def _(k):
        reduce2(k).wait()

    reduce1().wait()
    three = jnp.sum(r3[...].astype(F32), axis=0)
    two = jnp.sum(r2[...].astype(F32), axis=0)
    one = jnp.sum(r1[...].astype(F32), axis=0)
    four = jnp.sum(r4[...].astype(F32), axis=0) * (TOKENS**-0.5)
    dw_ref[...] = jnp.where(core == 0, four, pltpu.roll(four, 12, 0))
    low = iota((32, WIDE), 1) < 4 * HEAD
    cls = lane_head(128) & 3

    def whole(first, second, third, kept, scale):
        second = jnp.concatenate([second[0:8] + third, second[8:32]], axis=0)
        first = jnp.concatenate(
            [
                first[0:32] + jnp.where(low, second, 0.0),
                first[32:64] + jnp.where(low, 0.0, second),
                first[64:128],
            ],
            axis=0,
        )
        first = first * scale
        full = jnp.concatenate([jnp.where(cls == j, first, 0.0) for j in range(4)], axis=0)
        return (nn(pt_s[...], full.astype(BF16)) + kept[...]).astype(BF16)

    dk_ref[...] = whole(one[0:128], two[0:32], three[0:8], base_k, SCALE)
    dv_ref[...] = whole(one[128:256], two[32:64], three[8:16], base_v, 1.0)


def finish(a, b, c, d, e, out, dq, dk, dv, dw, sem):
    moves = [
        pltpu.make_async_copy(given, result, sem.at[n])
        for n, (given, result) in enumerate(((a, out), (b, dq), (c, dk), (d, dv)))
    ]
    for move in moves:
        move.start()
    dw[...] = e[0:12]
    for move in moves:
        move.wait()


def shards(queries, keys, values, w_out, d_out, slide_lengths):
    vmem = pl.BlockSpec(memory_space=pltpu.VMEM)
    anywhere = pl.BlockSpec(memory_space=pl.ANY)
    shape = jax.ShapeDtypeStruct

    def v(*dims, dtype=BF16):
        return pltpu.VMEM(dims, dtype)

    def sems(n):
        return pltpu.SemaphoreType.DMA((n,))

    scratch = [
        v(512, WIDE), v(512, WIDE), v(512, WIDE), v(WIDE, 768), v(512, WIDE),
        pltpu.SMEM((4,), jnp.int32), sems(6),
        v(512, 512), v(512, 512),
        v(WIDE, 512), v(WIDE, 512), v(WIDE, 512), v(WIDE, 512),
        v(1024, WIDE), v(256, WIDE), v(1024, WIDE), v(256, WIDE),
        v(2, 2, 256, WIDE), v(2, 8, 64, WIDE), v(2, 32, 16, WIDE),
        v(1024, WIDE), v(1024, WIDE), v(512, WIDE), v(512, WIDE),
        v(8, 512, 512), v(512, 1024), v(1024, 256),
        v(WIDE, 512, dtype=F32), v(8, 512, dtype=F32),
        v(8, 512, dtype=F32), v(8, 512, dtype=F32), v(8, 1024, dtype=F32), v(8, 256, dtype=F32),
        v(WIDE, 512, dtype=F32), v(WIDE, 512, dtype=F32), v(WIDE, 512, dtype=F32),
        v(512, WIDE, dtype=F32), v(512, WIDE, dtype=F32),
        v(512, WIDE), v(512, WIDE), v(512, WIDE), v(512, WIDE),
        v(2, 2, 256, WIDE), v(2, 8, 64, WIDE), v(2, 32, 16, WIDE), v(2, 32, 16, WIDE),
        v(2, 256, WIDE), v(8, 64, WIDE), v(32, 16, WIDE), v(32, 16, WIDE),
        v(2, 256, WIDE), v(8, 64, WIDE), v(32, 16, WIDE), v(32, 16, WIDE),
        v(2, 256, WIDE), v(8, 64, WIDE), v(32, 16, WIDE), v(32, 16, WIDE),
        sems(2), sems(2),
        sems(2), sems(2), sems(8), sems(8), sems(32), sems(32),
        sems(2), sems(2), sems(8), sems(8), sems(32), sems(32), sems(32), sems(32),
    ]
    out, dq, dk, dv, dw = pl.pallas_call(
        kernel,
        out_shape=[shape((ROWS, WIDE), BF16)] * 4 + [shape((16, WIDE), F32)],
        in_specs=[anywhere] * 6,
        out_specs=[vmem] * 5,
        scratch_shapes=scratch,
        compiler_params=pltpu.CompilerParams(
            collective_id=0, has_side_effects=True, vmem_limit_bytes=54_800_000
        ),
    )(queries, keys, values, w_out, d_out, slide_lengths)
    out, dq, dk, dv, dw = pl.pallas_call(
        finish,
        out_shape=[shape((ROWS, WIDE), BF16)] * 4 + [shape((12, WIDE), F32)],
        in_specs=[anywhere] * 4 + [vmem],
        out_specs=[anywhere] * 4 + [vmem],
        scratch_shapes=[sems(4)],
        compiler_params=pltpu.CompilerParams(vmem_limit_bytes=4 * 1024 * 1024),
    )(out, dq, dk, dv, dw)
    return out, dq, dk, dv, dw.T


def solution(mesh):
    both = P("seq", "head")
    return jax.shard_map(
        shards,
        mesh=mesh,
        in_specs=(both, both, both, P("head", None), both, P()),
        out_specs=(both, both, both, both, P("head", "seq")),
        check_vma=False,
    )
```

```python
import jax
import jax.numpy as jnp
from jax import lax
from jax.experimental import pallas as pl
from jax.experimental.pallas import tpu as pltpu
from jax.sharding import PartitionSpec as P

TOKENS = 32768
HEAD = 48
ROWS = 512
WIDE = 384
HEADS = 8
NEG = -1e30
SCALE = HEAD**-0.5
LOG2E = 1.4426950408889634
C2 = SCALE * LOG2E
FAR = 1 << 30
F32 = jnp.float32
BF16 = jnp.bfloat16
MESH = pl.DeviceIdType.MESH


def nn(a, b):
    return lax.dot_general(a, b, (((1,), (0,)), ((), ())), preferred_element_type=F32)


def nt(a, b):
    return lax.dot_general(a, b, (((1,), (1,)), ((), ())), preferred_element_type=F32)


def tn(a, b):
    return lax.dot_general(a, b, (((0,), (0,)), ((), ())), preferred_element_type=F32)


def iota(shape, dim):
    return lax.broadcasted_iota(jnp.int32, shape, dim)


def token_of(a, g):
    return (a >> 7) + 4 * ((((a >> 5) & 3) + 2 * g) & 3) + 16 * ((a >> 3) & 3) + 64 * (a & 7)


def lane_head(rows):
    lane = iota((rows, WIDE), 1)
    head = jnp.zeros_like(lane)
    for i in range(1, HEADS):
        head = head + (lane >= HEAD * i).astype(jnp.int32)
    return head


def compact1(x):
    cls = lane_head(128) & 3
    y = jnp.where(cls == 0, x[0:128], x[128:256])
    y = jnp.where(cls == 2, x[256:384], y)
    return jnp.where(cls == 3, x[384:512], y)


def compact2(x1):
    return jnp.where(iota((32, WIDE), 1) < 4 * HEAD, x1[0:32], x1[32:64])


def stacked(x, n):
    rows = HEADS * n
    shift = n.bit_length() - 1
    own = (iota((rows, WIDE), 0) >> shift) == lane_head(rows)
    return jnp.where(own, jnp.concatenate([x] * HEADS, axis=0), 0.0).astype(BF16)


def to_tile(x, i):
    t, at, to = i // 4, 32 * (i % 4), 32 * (i // 4)
    tile = x[:, 128 * t : 128 * t + 128]
    shift = (to - at) % 128
    return pltpu.roll(tile, shift, 1) if shift else tile


def from_tiles(tiles):
    halves = []
    for t in range(2):
        lane = iota(tiles[0].shape, 1)
        half = None
        for i in range(4 * t, 4 * t + 4):
            at, to = 32 * (i % 4), 32 * (i // 4)
            shift = (at - to) % 128
            moved = pltpu.roll(tiles[i], shift, 1) if shift else tiles[i]
            half = moved if half is None else jnp.where((lane >> 5) == (i % 4), moved, half)
        halves.append(half)
    return jnp.concatenate(halves, axis=1)


def kernel(
    q_in, k_in, v_in, w_in, d_in, len_in,
    out_ref, dq_ref, dk_ref, dv_ref, dw_ref,
    q_ref, k_ref, v_ref, w_ref, d_ref, len_ref, in_sem,
    p_s, pt_s, qt_s, kt_s, vt_s, dt_s, qx1, qx2, dx1, dx2,
    g1, g2, g3, kg23, vg23, kg1, vg1, p0s, p1s, p23s,
    a0, m0, lse_s, del_s, m1s, m23s, dqt, dkt, dvt, base_k, base_v,
    doth, att_s, po_send, po_recv,
    x1, x2, x3, x4, y1, y2, y3, y4, z1, z2, z3, z4, r1, r2, r3, r4, q3, q4, r5, r6,
    one_send, one_recv, s1, t1, s2, t2, s3, t3, u1, w1, u2, w2, u3, w3, u4, w4,
):
    seq = lax.axis_index("seq")
    g = lax.axis_index("head")
    chip = seq // 2
    core = seq % 2
    partner = {"seq": chip * 2 + (1 - core), "head": g}
    across = {"seq": seq, "head": 1 - g}

    def chip_at(c):
        return {"seq": c * 2 + core, "head": g}

    base1, base2 = (chip // 2) * 2, (chip // 8) * 8
    me1, me2, me3 = chip - base1, chip - base2, chip
    z, zrow = chip % 4, chip // 4
    row_low = zrow + 1 - 2 * (zrow % 2)

    def in_row(k):
        return chip_at(4 * zrow + (z + k) % 4)

    def other_row(k):
        return (zrow + k) % 8

    loads = [
        pltpu.make_async_copy(a, b, in_sem.at[n])
        for n, (a, b) in enumerate(
            ((k_in, k_ref), (v_in, v_ref), (q_in, q_ref), (d_in, d_ref), (w_in, w_ref), (len_in, len_ref))
        )
    ]
    for load in loads:
        load.start()
    barrier = pltpu.get_barrier_semaphore()
    pl.semaphore_signal(barrier, inc=1, device_id=partner, device_id_type=MESH)
    pl.semaphore_signal(barrier, inc=1, device_id=across, device_id_type=MESH)

    for k in range(1, 4):
        pl.semaphore_signal(barrier, inc=1, device_id=in_row(k), device_id_type=MESH)
        pl.semaphore_signal(
            barrier, inc=1, device_id=chip_at(4 * row_low + (z + k) % 4), device_id_type=MESH
        )
    for k in range(1, 8):
        pl.semaphore_signal(
            barrier, inc=1, device_id=chip_at(4 * other_row(k) + z), device_id_type=MESH
        )

    p_s[...] = (iota((ROWS, ROWS), 1) == token_of(iota((ROWS, ROWS), 0), g)).astype(F32).astype(BF16)
    pt_s[...] = (iota((ROWS, ROWS), 0) == token_of(iota((ROWS, ROWS), 1), g)).astype(F32).astype(BF16)

    def levels_of(x):
        y1_ = compact1(nn(p_s[...], x))
        y2_ = compact2(y1_)
        return y1_, y2_, y2_[0:8]

    loads[0].wait()
    ka, kb, kc = levels_of(k_ref[...])
    loads[1].wait()
    va, vb, vc = levels_of(v_ref[...])
    g1[core, me1, 0:128] = ka.astype(BF16)
    g1[core, me1, 128:256] = va.astype(BF16)
    g2[core, me2, 0:32] = kb.astype(BF16)
    g2[core, me2, 32:64] = vb.astype(BF16)
    g3[core, me3] = jnp.concatenate([kc, vc], axis=0).astype(BF16)

    pl.semaphore_wait(barrier, 15)

    def remote(src, dst, ss, rs, dev):
        return pltpu.make_async_remote_copy(
            src_ref=src, dst_ref=dst, send_sem=ss, recv_sem=rs, device_id=dev, device_id_type=MESH
        )

    def gather3(k):
        return remote(g3.at[core, me3], g3.at[core, me3], s3.at[k], t3.at[k], in_row(k))

    def gather4(k):
        row = g3.at[core, pl.ds(4 * zrow, 4)]
        return remote(row, row, s3.at[8 + k], t3.at[8 + k], chip_at(4 * other_row(k) + z))

    def gather2(k):
        return remote(
            g2.at[core, me2], g2.at[core, me2], s2.at[k], t2.at[k], chip_at(base2 + (me2 + k) % 8)
        )

    def gather1():
        return remote(g1.at[core, me1], g1.at[core, me1], s1.at[1], t1.at[1], chip_at(base1 + 1 - me1))

    for k in range(1, 4):
        gather3(k).start()

    gather1().start()

    @pl.loop(1, 8)
    def _(k):
        gather2(k).start()


    for k in range(1, 4):
        gather3(k).wait()
    for k in range(1, 8):
        gather4(k).start()

    loads[3].wait()
    send_d = remote(d_ref, doth, one_send.at[0], one_recv.at[0], across)
    send_d.start()

    loads[2].wait()
    qa, qb, _ = levels_of(q_ref[...])
    qx1[...] = stacked(qa, 128)
    qx2[...] = stacked(qb, 32)
    kt_s[...] = tn(k_ref[...], pt_s[...]).astype(BF16)
    qt_s[...] = tn(q_ref[...], pt_s[...]).astype(BF16)
    vt_s[...] = tn(v_ref[...], pt_s[...]).astype(BF16)

    loads[5].wait()
    start1 = len_ref[0]
    start2 = start1 + len_ref[1]
    start3 = start2 + len_ref[2]

    def ids_of(pos):
        return (
            (pos >= start1).astype(jnp.int32)
            + (pos >= start2).astype(jnp.int32)
            + (pos >= start3).astype(jnp.int32)
        )

    here = seq * ROWS
    id_k = ids_of(here + token_of(iota((ROWS, 1), 0), g))
    id_q = ids_of(here + token_of(iota((1, ROWS), 1), g))

    def head_rows(i):
        return pl.ds(pl.multiple_of(i * HEAD, 16), HEAD)

    def head_forward(i):
        rows = head_rows(i)
        s = tn(kt_s[rows, :], qt_s[rows, :])
        s = jnp.where(id_k == id_q, s, NEG)
        top = jnp.max(s, axis=0, keepdims=True)
        p = jnp.exp2((s - top) * C2)
        total = jnp.sum(p, axis=0, keepdims=True)
        m0[pl.ds(i, 1), :] = top
        lse_s[pl.ds(i, 1), :] = top * C2 + jnp.log2(total)
        pb = p.astype(BF16)
        p0s[i] = pb
        a0[rows, :] = nn(vt_s[rows, :], pb) / total

    pl.loop(0, 4, unroll=2)(head_forward)

    gather1().wait()
    core1 = remote(g1.at[core], g1.at[core], s1.at[0], t1.at[0], partner)
    core1.start()
    pl.loop(4, HEADS, unroll=2)(head_forward)
    for k in range(1, 8):
        gather4(k).wait()
    core3 = remote(g3.at[core], g3.at[core], s3.at[0], t3.at[0], partner)
    core3.start()

    def slide_range(pos):
        lo = jnp.where(pos >= start1, start1, 0)
        lo = jnp.where(pos >= start2, start2, lo)
        lo = jnp.where(pos >= start3, start3, lo)
        hi = jnp.where(pos < start3, start3, TOKENS)
        hi = jnp.where(pos < start2, start2, hi)
        hi = jnp.where(pos < start1, start1, hi)
        return lo, hi

    def masked(s, key_pos, lo, hi):
        return jnp.where((key_pos >= lo) & (key_pos < hi), s, NEG)

    core1.wait()
    row = iota((512, 1), 0)
    kg1[...] = g1[:, :, 0:128].reshape(512, WIDE)
    vg1[...] = g1[:, :, 128:256].reshape(512, WIDE)
    colb = iota((1, 1024), 1)
    offb = (colb >> 7) & 3

    def spread1(j):
        return 4 * ((((j >> 5) & 3) + 2 * g) & 3) + 16 * ((j >> 3) & 3) + 64 * (j & 7)

    lo1, hi1 = slide_range(here + offb + spread1(colb & 127))
    lo1, hi1 = lo1 - offb, hi1 - offb
    pos1 = 512 * (2 * (base1 + ((row >> 7) & 1)) + (row >> 8)) + spread1(row & 127)
    top1, sum1, acc1 = [], [], []
    for half in range(2):
        c = slice(512 * half, 512 * half + 512)
        w = slice(128 * half, 128 * half + 256)
        sc = masked(nt(kg1[:, w], qx1[c, w]), pos1, lo1[:, c], hi1[:, c])
        top1.append(jnp.max(sc, axis=0, keepdims=True))
        pc = jnp.exp2((sc - top1[half]) * C2)
        sum1.append(jnp.sum(pc, axis=0, keepdims=True))
        p1s[:, c] = pc.astype(BF16)
        m1s[:, c] = jnp.broadcast_to(top1[half], (8, 512))
        acc1.append(tn(vg1[:, w], p1s[:, c]))

    @pl.loop(1, 8)
    def _(k):
        gather2(k).wait()

    core2 = remote(g2.at[core], g2.at[core], s2.at[0], t2.at[0], partner)
    core2.start()

    core3.wait()
    core2.wait()
    three = g3[...].astype(F32).reshape(64, 16, WIDE)
    kg23[0:512] = g2[:, :, 0:32].reshape(512, WIDE)
    vg23[0:512] = g2[:, :, 32:64].reshape(512, WIDE)
    kg23[512:1024] = three[:, 0:8].reshape(512, WIDE).astype(BF16)
    vg23[512:1024] = three[:, 8:16].reshape(512, WIDE).astype(BF16)

    col = iota((1, 256), 1)
    inner = col & 31
    off = 8 * g + (col >> 5)
    lo, hi = slide_range(here + off + 16 * (inner >> 3) + 64 * (inner & 7))
    lo, hi = lo - off, hi - off
    pos2 = 512 * (2 * (base2 + ((row >> 5) & 7)) + (row >> 8)) + 16 * ((row >> 3) & 3) + 64 * (row & 7)
    pos3 = 512 * (2 * ((row >> 3) & 31) + (row >> 8)) + 64 * (row & 7)
    sa = masked(nt(kg23[0:512], qx2[...]), pos2, lo, hi)
    sb = masked(nt(kg23[512:1024], qx2[...]), pos3, jnp.where(inner < 8, lo, FAR), hi)
    top23 = jnp.maximum(jnp.max(sa, axis=0, keepdims=True), jnp.max(sb, axis=0, keepdims=True))
    pa = jnp.exp2((sa - top23) * C2)
    pb3 = jnp.exp2((sb - top23) * C2)
    sum23 = jnp.sum(pa, axis=0, keepdims=True) + jnp.sum(pb3, axis=0, keepdims=True)
    p23s[0:512] = pa.astype(BF16)
    p23s[512:1024] = pb3.astype(BF16)
    m23s[...] = jnp.broadcast_to(top23, (8, 256))
    acc23 = tn(vg23[...], p23s[...])

    st23 = jnp.broadcast_to(top23, (8, 256))
    su23 = jnp.broadcast_to(sum23, (8, 256))
    lane8 = iota((8, 128), 1) >> 5
    lane48 = iota((HEAD, 128), 1) >> 5
    for i in range(HEADS):
        r = slice(HEAD * i, HEAD * i + HEAD)
        c = slice(128 * (i % 4), 128 * (i % 4) + 128)
        half = i // 4
        rr = slice(HEAD * i - 128 * half, HEAD * i - 128 * half + HEAD)
        two = jnp.where(lane8 == i // 4, to_tile(st23, i), NEG)[0:1]
        two_sum = jnp.where(lane8 == i // 4, to_tile(su23, i), 0.0)[0:1]
        two_acc = jnp.where(lane48 == i // 4, to_tile(acc23[r], i), 0.0)
        zero = lse_s[i : i + 1, c]
        one = top1[half][:, c] * C2
        two = two * C2
        new = jnp.maximum(jnp.maximum(zero, one), two)
        f0 = jnp.exp2(zero - new)
        f1 = jnp.exp2(one - new)
        f2 = jnp.exp2(two - new)
        l_new = f0 + sum1[half][:, c] * f1 + two_sum * f2
        a_new = (a0[r, c] * f0 + acc1[half][rr, c] * f1 + two_acc * f2) / l_new
        a0[r, c] = a_new
        lse_s[i : i + 1, c] = new + jnp.log2(l_new)

    att_t = a0[...].astype(BF16)
    att = nt(pt_s[...], att_t).astype(BF16)
    att_s[...] = att
    loads[4].wait()
    own = pl.ds(pl.multiple_of(g * WIDE, 128), WIDE)
    other = pl.ds(pl.multiple_of((1 - g) * WIDE, 128), WIDE)
    po_send[...] = nn(att, w_ref[:, other]).astype(BF16)

    def send_o(part):
        rows = pl.ds(256 * part, 256)
        n = 1 + part
        return remote(po_send.at[rows], po_recv.at[rows], one_send.at[n], one_recv.at[n], across)

    send_o(0).start()

    send_d.wait()
    for part, block in ((g, d_ref), (1 - g, doth)):
        term = tn(block[...], att)
        for c in range(16):
            x4[0, c % 4, 4 * part + c // 4] = term[24 * c : 24 * c + 16].astype(BF16)
            x4[1, c % 4, 4 * part + c // 4] = term[24 * c + 8 : 24 * c + 24].astype(BF16)
    swap4 = remote(x4.at[1 - core], y4, u4.at[0], w4.at[0], partner)
    swap4.start()
    d_att = (nt(d_ref[...], w_ref[:, own]) + nt(doth[...], w_ref[:, other])).astype(BF16)
    dt = tn(d_att, pt_s[...])
    dt_s[...] = dt.astype(BF16)
    da, db, _ = levels_of(d_att)
    dx1[...] = stacked(da, 128)
    dx2[...] = stacked(db, 32)

    prod = dt_s[...].astype(F32) * att_t.astype(F32)
    for i in range(HEADS):
        del_s[i : i + 1, :] = jnp.sum(prod[HEAD * i : HEAD * i + HEAD], axis=0, keepdims=True)

    def tiles_of(ref):
        return [
            jnp.broadcast_to(ref[i : i + 1, 128 * (i % 4) : 128 * (i % 4) + 128], (8, 128))
            for i in range(HEADS)
        ]

    lse_tiles, del_tiles = tiles_of(lse_s), tiles_of(del_s)
    lse23 = from_tiles(lse_tiles)[0:1]
    del23 = from_tiles(del_tiles)[0:1]
    p = p23s[...].astype(F32) * jnp.exp2(m23s[0:1] * C2 - lse23)
    ds = (p * (nt(vg23[...], dx2[...]) - del23)).astype(BF16)
    dk23 = nn(ds, qx2[...])
    dv23 = nn(p.astype(BF16), dx2[...])
    dq23 = tn(kg23[...], ds)
    x2[:, :, 0:32] = dk23[0:512].reshape(2, 8, 32, WIDE).astype(BF16)
    x2[:, :, 32:64] = dv23[0:512].reshape(2, 8, 32, WIDE).astype(BF16)
    x3[...] = jnp.concatenate(
        [dk23[512:1024].reshape(2, 32, 8, WIDE), dv23[512:1024].reshape(2, 32, 8, WIDE)], axis=2
    ).astype(BF16)
    swap3 = remote(x3.at[1 - core], y3, u3.at[0], w3.at[0], partner)
    swap3.start()
    swap2 = remote(x2.at[1 - core], y2, u2.at[0], w2.at[0], partner)
    swap2.start()

    swap4.wait()
    z4[...] = (x4[core].astype(F32) + y4[...].astype(F32)).astype(BF16)
    r4[z] = z4[z]

    def reduce4(k):
        return remote(z4.at[(z + k) % 4], r4.at[z], u4.at[k], w4.at[k], in_row(k))

    def reduce6(k):
        to = other_row(k)
        return remote(q4.at[to], r6.at[zrow], u4.at[8 + k], w4.at[8 + k], chip_at(4 * to + z))

    for k in range(1, 4):
        reduce4(k).start()

    lse1 = jnp.concatenate([t[0:1] for t in lse_tiles], axis=1)
    del1 = jnp.concatenate([t[0:1] for t in del_tiles], axis=1)
    dk1, dv1, dq1 = [], [], []
    for half in range(2):
        c = slice(512 * half, 512 * half + 512)
        w = slice(128 * half, 128 * half + 256)
        p = p1s[:, c].astype(F32) * jnp.exp2(m1s[0:1, c] * C2 - lse1[:, c])
        ds = (p * (nt(vg1[:, w], dx1[c, w]) - del1[:, c])).astype(BF16)
        dk1.append(nn(ds, qx1[c, w]))
        dv1.append(nn(p.astype(BF16), dx1[c, w]))
        dq1.append(tn(kg1[:, w], ds))

    def joined(a, b):
        return jnp.concatenate([a[:, 0:128], a[:, 128:256] + b[:, 0:128], b[:, 128:256]], axis=1)

    dk1, dv1 = joined(*dk1), joined(*dv1)
    x1[:, :, 0:128] = dk1.reshape(2, 2, 128, WIDE).astype(BF16)
    x1[:, :, 128:256] = dv1.reshape(2, 2, 128, WIDE).astype(BF16)
    swap1 = remote(x1.at[1 - core], y1, u1.at[0], w1.at[0], partner)
    swap1.start()

    swap3.wait()
    z3[...] = (x3[core].astype(F32) + y3[...].astype(F32)).astype(BF16)
    swap2.wait()
    z2[...] = (x2[core].astype(F32) + y2[...].astype(F32)).astype(BF16)
    r3[zrow] = z3[pl.ds(4 * zrow, 4)]
    r2[me2] = z2[me2]
    def reduce3(k):
        to = other_row(k)
        return remote(
            z3.at[pl.ds(4 * to, 4)], r3.at[zrow], u3.at[k], w3.at[k], chip_at(4 * to + z)
        )

    def reduce5(k):
        return remote(q3.at[(z + k) % 4], r5.at[z], u3.at[8 + k], w3.at[8 + k], in_row(k))

    def reduce2(k):
        to = (me2 + k) % 8
        return remote(z2.at[to], r2.at[me2], u2.at[k], w2.at[k], chip_at(base2 + to))

    def reduce1():
        return remote(z1.at[1 - me1], r1.at[me1], u1.at[1], w1.at[1], chip_at(base1 + 1 - me1))

    for k in range(1, 8):
        reduce3(k).start()

    @pl.loop(1, 8)
    def _(k):
        reduce2(k).start()

    send_o(1).start()

    a0[...] = jnp.concatenate(
        [jnp.exp2(m0[...] * C2 - lse_s[...])] * (WIDE // HEADS), axis=0
    )

    def head_back(i):
        rows = head_rows(i)
        p = p0s[i].astype(F32) * a0[pl.ds(i, 1), :]
        pb = p.astype(BF16)
        dp = tn(vt_s[rows, :], dt_s[rows, :])
        ds = (p * (dp - del_s[pl.ds(i, 1), :])).astype(BF16)
        dqt[rows, :] = nn(kt_s[rows, :], ds)
        dkt[rows, :] = nt(qt_s[rows, :], ds)
        dvt[rows, :] = nt(dt_s[rows, :], pb)

    pl.loop(0, 2, unroll=2)(head_back)
    swap1.wait()
    z1[...] = (x1[core].astype(F32) + y1[...].astype(F32)).astype(BF16)
    r1[me1] = z1[me1]
    reduce1().start()
    for k in range(1, 4):
        reduce4(k).wait()
    q4[...] = jnp.sum(r4[...].astype(F32), axis=0).astype(BF16)
    r6[zrow] = q4[zrow]
    for k in range(1, 8):
        reduce6(k).start()
    pl.loop(2, 6, unroll=2)(head_back)
    for k in range(1, 8):
        reduce3(k).wait()
    q3[...] = jnp.sum(r3[...].astype(F32), axis=0).astype(BF16)
    r5[z] = q3[z]
    for k in range(1, 4):
        reduce5(k).start()
    pl.loop(6, 8, unroll=2)(head_back)

    for i in range(HEADS):
        r = slice(HEAD * i, HEAD * i + HEAD)
        c = slice(128 * (i % 4), 128 * (i % 4) + 128)
        half = i // 4
        rr = slice(HEAD * i - 128 * half, HEAD * i - 128 * half + HEAD)
        two = jnp.where(lane48 == half, to_tile(dq23[r], i), 0.0)
        dqt[r, c] = dqt[r, c] + dq1[half][rr, c] + two
    dq_ref[...] = nt(pt_s[...], (dqt[...] * SCALE).astype(BF16)).astype(BF16)

    for level0, scale, kept in ((dkt, SCALE, base_k), (dvt, 1.0, base_v)):
        kept[...] = nt(pt_s[...], (level0[...] * scale).astype(BF16))

    send_o(0).wait()
    send_o(1).wait()
    out_ref[...] = (nn(att_s[...], w_ref[:, own]) + po_recv[...].astype(F32)).astype(BF16)

    for k in range(1, 8):
        reduce6(k).wait()
    for k in range(1, 4):
        reduce5(k).wait()

    @pl.loop(1, 8)
    def _(k):
        reduce2(k).wait()

    reduce1().wait()
    three = jnp.sum(r5[...].astype(F32), axis=0)
    two = jnp.sum(r2[...].astype(F32), axis=0)
    one = jnp.sum(r1[...].astype(F32), axis=0)
    four = jnp.sum(r6[...].astype(F32), axis=0) * (TOKENS**-0.5)
    dw_ref[...] = jnp.where(core == 0, four, pltpu.roll(four, 12, 0))
    low = iota((32, WIDE), 1) < 4 * HEAD
    cls = lane_head(128) & 3

    def whole(first, second, third, kept, scale):
        second = jnp.concatenate([second[0:8] + third, second[8:32]], axis=0)
        first = jnp.concatenate(
            [
                first[0:32] + jnp.where(low, second, 0.0),
                first[32:64] + jnp.where(low, 0.0, second),
                first[64:128],
            ],
            axis=0,
        )
        first = first * scale
        full = jnp.concatenate([jnp.where(cls == j, first, 0.0) for j in range(4)], axis=0)
        return (nn(pt_s[...], full.astype(BF16)) + kept[...]).astype(BF16)

    dk_ref[...] = whole(one[0:128], two[0:32], three[0:8], base_k, SCALE)
    dv_ref[...] = whole(one[128:256], two[32:64], three[8:16], base_v, 1.0)


def finish(a, b, c, d, e, out, dq, dk, dv, dw, sem):
    moves = [
        pltpu.make_async_copy(given, result, sem.at[n])
        for n, (given, result) in enumerate(((a, out), (b, dq), (c, dk), (d, dv)))
    ]
    for move in moves:
        move.start()
    dw[...] = e[0:12]
    for move in moves:
        move.wait()


def shards(queries, keys, values, w_out, d_out, slide_lengths):
    vmem = pl.BlockSpec(memory_space=pltpu.VMEM)
    anywhere = pl.BlockSpec(memory_space=pl.ANY)
    shape = jax.ShapeDtypeStruct

    def v(*dims, dtype=BF16):
        return pltpu.VMEM(dims, dtype)

    def sems(n):
        return pltpu.SemaphoreType.DMA((n,))

    scratch = [
        v(512, WIDE), v(512, WIDE), v(512, WIDE), v(WIDE, 768), v(512, WIDE),
        pltpu.SMEM((4,), jnp.int32), sems(6),
        v(512, 512), v(512, 512),
        v(WIDE, 512), v(WIDE, 512), v(WIDE, 512), v(WIDE, 512),
        v(1024, WIDE), v(256, WIDE), v(1024, WIDE), v(256, WIDE),
        v(2, 2, 256, WIDE), v(2, 8, 64, WIDE), v(2, 32, 16, WIDE),
        v(1024, WIDE), v(1024, WIDE), v(512, WIDE), v(512, WIDE),
        v(8, 512, 512), v(512, 1024), v(1024, 256),
        v(WIDE, 512, dtype=F32), v(8, 512, dtype=F32),
        v(8, 512, dtype=F32), v(8, 512, dtype=F32), v(8, 1024, dtype=F32), v(8, 256, dtype=F32),
        v(WIDE, 512, dtype=F32), v(WIDE, 512, dtype=F32), v(WIDE, 512, dtype=F32),
        v(512, WIDE, dtype=F32), v(512, WIDE, dtype=F32),
        v(512, WIDE), v(512, WIDE), v(512, WIDE), v(512, WIDE),
        v(2, 2, 256, WIDE), v(2, 8, 64, WIDE), v(2, 32, 16, WIDE), v(2, 4, 8, 16, WIDE),
        v(2, 256, WIDE), v(8, 64, WIDE), v(32, 16, WIDE), v(4, 8, 16, WIDE),
        v(2, 256, WIDE), v(8, 64, WIDE), v(32, 16, WIDE), v(4, 8, 16, WIDE),
        v(2, 256, WIDE), v(8, 64, WIDE), v(8, 4, 16, WIDE), v(4, 8, 16, WIDE),
        v(4, 16, WIDE), v(8, 16, WIDE), v(4, 16, WIDE), v(8, 16, WIDE),
        sems(3), sems(3),
        sems(2), sems(2), sems(8), sems(8), sems(32), sems(32),
        sems(2), sems(2), sems(8), sems(8), sems(32), sems(32), sems(32), sems(32),
    ]
    out, dq, dk, dv, dw = pl.pallas_call(
        kernel,
        out_shape=[shape((ROWS, WIDE), BF16)] * 4 + [shape((16, WIDE), F32)],
        in_specs=[anywhere] * 6,
        out_specs=[vmem] * 5,
        scratch_shapes=scratch,
        compiler_params=pltpu.CompilerParams(
            collective_id=0, has_side_effects=True, vmem_limit_bytes=54_800_000
        ),
    )(queries, keys, values, w_out, d_out, slide_lengths)
    out, dq, dk, dv, dw = pl.pallas_call(
        finish,
        out_shape=[shape((ROWS, WIDE), BF16)] * 4 + [shape((12, WIDE), F32)],
        in_specs=[anywhere] * 4 + [vmem],
        out_specs=[anywhere] * 4 + [vmem],
        scratch_shapes=[sems(4)],
        compiler_params=pltpu.CompilerParams(vmem_limit_bytes=4 * 1024 * 1024),
    )(out, dq, dk, dv, dw)
    return out, dq, dk, dv, dw.T


def solution(mesh):
    both = P("seq", "head")
    return jax.shard_map(
        shards,
        mesh=mesh,
        in_specs=(both, both, both, P("head", None), both, P()),
        out_specs=(both, both, both, both, P("head", "seq")),
        check_vma=False,
    )
```

```python
import jax
import jax.numpy as jnp
from jax import lax
from jax.experimental import pallas as pl
from jax.experimental.pallas import tpu as pltpu
from jax.sharding import PartitionSpec as P

TOKENS = 32768
HEAD = 48
ROWS = 512
WIDE = 384
HEADS = 8
NEG = -1e30
SCALE = HEAD**-0.5
LOG2E = 1.4426950408889634
C2 = SCALE * LOG2E
FAR = 1 << 30
F32 = jnp.float32
BF16 = jnp.bfloat16
MESH = pl.DeviceIdType.MESH


def nn(a, b):
    return lax.dot_general(a, b, (((1,), (0,)), ((), ())), preferred_element_type=F32)


def nt(a, b):
    return lax.dot_general(a, b, (((1,), (1,)), ((), ())), preferred_element_type=F32)


def tn(a, b):
    return lax.dot_general(a, b, (((0,), (0,)), ((), ())), preferred_element_type=F32)


def iota(shape, dim):
    return lax.broadcasted_iota(jnp.int32, shape, dim)


def token_of(a, g):
    return (a >> 7) + 4 * ((((a >> 5) & 3) + 2 * g) & 3) + 16 * ((a >> 3) & 3) + 64 * (a & 7)


def lane_head(rows):
    lane = iota((rows, WIDE), 1)
    head = jnp.zeros_like(lane)
    for i in range(1, HEADS):
        head = head + (lane >= HEAD * i).astype(jnp.int32)
    return head


def compact1(x):
    cls = lane_head(128) & 3
    y = jnp.where(cls == 0, x[0:128], x[128:256])
    y = jnp.where(cls == 2, x[256:384], y)
    return jnp.where(cls == 3, x[384:512], y)


def compact2(x1):
    return jnp.where(iota((32, WIDE), 1) < 4 * HEAD, x1[0:32], x1[32:64])


def stacked(x, n):
    rows = HEADS * n
    shift = n.bit_length() - 1
    own = (iota((rows, WIDE), 0) >> shift) == lane_head(rows)
    return jnp.where(own, jnp.concatenate([x] * HEADS, axis=0), 0.0).astype(BF16)


def to_tile(x, i):
    t, at, to = i // 4, 32 * (i % 4), 32 * (i // 4)
    tile = x[:, 128 * t : 128 * t + 128]
    shift = (to - at) % 128
    return pltpu.roll(tile, shift, 1) if shift else tile


def from_tiles(tiles):
    halves = []
    for t in range(2):
        lane = iota(tiles[0].shape, 1)
        half = None
        for i in range(4 * t, 4 * t + 4):
            at, to = 32 * (i % 4), 32 * (i // 4)
            shift = (at - to) % 128
            moved = pltpu.roll(tiles[i], shift, 1) if shift else tiles[i]
            half = moved if half is None else jnp.where((lane >> 5) == (i % 4), moved, half)
        halves.append(half)
    return jnp.concatenate(halves, axis=1)


def kernel(
    q_in, k_in, v_in, w_in, d_in, len_in,
    out_ref, dq_ref, dk_ref, dv_ref, dw_ref,
    q_ref, k_ref, v_ref, w_ref, d_ref, len_ref, in_sem,
    p_s, pt_s, qt_s, kt_s, vt_s, dt_s, qx1, qx2, dx1, dx2,
    g1, g2, g3, kg23, vg23, kg1, vg1, p0s, p1s, p23s,
    a0, m0, lse_s, del_s, m1s, m23s, dqt, dkt, dvt, base_k, base_v,
    doth, att_s, po_send, po_recv,
    x1, x2, x3, x4, y1, y2, y3, y4, z1, z2, z3, z4, r1, r2, r3, r4, q3, q4, r5, r6,
    one_send, one_recv, s1, t1, s2, t2, s3, t3, u1, w1, u2, w2, u3, w3, u4, w4,
):
    seq = lax.axis_index("seq")
    g = lax.axis_index("head")
    chip = seq // 2
    core = seq % 2
    partner = {"seq": chip * 2 + (1 - core), "head": g}
    across = {"seq": seq, "head": 1 - g}

    def chip_at(c):
        return {"seq": c * 2 + core, "head": g}

    base1, base2 = (chip // 2) * 2, (chip // 8) * 8
    me1, me2, me3 = chip - base1, chip - base2, chip
    z, zrow = chip % 4, chip // 4
    row_low = zrow + 1 - 2 * (zrow % 2)

    def in_row(k):
        return chip_at(4 * zrow + (z + k) % 4)

    def other_row(k):
        return (zrow + k) % 8

    loads = [
        pltpu.make_async_copy(a, b, in_sem.at[n])
        for n, (a, b) in enumerate(
            ((k_in, k_ref), (v_in, v_ref), (q_in, q_ref), (d_in, d_ref), (w_in, w_ref), (len_in, len_ref))
        )
    ]
    loads[0].start()
    loads[1].start()
    barrier = pltpu.get_barrier_semaphore()
    pl.semaphore_signal(barrier, inc=1, device_id=partner, device_id_type=MESH)
    pl.semaphore_signal(barrier, inc=1, device_id=across, device_id_type=MESH)

    for k in range(1, 4):
        pl.semaphore_signal(barrier, inc=1, device_id=in_row(k), device_id_type=MESH)
        pl.semaphore_signal(
            barrier, inc=1, device_id=chip_at(4 * row_low + (z + k) % 4), device_id_type=MESH
        )
    for k in range(1, 8):
        pl.semaphore_signal(
            barrier, inc=1, device_id=chip_at(4 * other_row(k) + z), device_id_type=MESH
        )

    p_s[...] = (iota((ROWS, ROWS), 1) == token_of(iota((ROWS, ROWS), 0), g)).astype(F32).astype(BF16)

    def levels_of(x):
        y1_ = compact1(nn(p_s[...], x))
        y2_ = compact2(y1_)
        return y1_, y2_, y2_[0:8]

    loads[0].wait()
    ka, kb, kc = levels_of(k_ref[...])
    loads[1].wait()
    for n in (2, 3, 4, 5):
        loads[n].start()
    va, vb, vc = levels_of(v_ref[...])
    g1[core, me1, 0:128] = ka.astype(BF16)
    g1[core, me1, 128:256] = va.astype(BF16)
    g2[core, me2, 0:32] = kb.astype(BF16)
    g2[core, me2, 32:64] = vb.astype(BF16)
    g3[core, me3] = jnp.concatenate([kc, vc], axis=0).astype(BF16)

    pl.semaphore_wait(barrier, 15)

    def remote(src, dst, ss, rs, dev):
        return pltpu.make_async_remote_copy(
            src_ref=src, dst_ref=dst, send_sem=ss, recv_sem=rs, device_id=dev, device_id_type=MESH
        )

    def gather3(k):
        return remote(g3.at[core, me3], g3.at[core, me3], s3.at[k], t3.at[k], in_row(k))

    def gather4(k):
        row = g3.at[core, pl.ds(4 * zrow, 4)]
        return remote(row, row, s3.at[8 + k], t3.at[8 + k], chip_at(4 * other_row(k) + z))

    def gather2(k):
        return remote(
            g2.at[core, me2], g2.at[core, me2], s2.at[k], t2.at[k], chip_at(base2 + (me2 + k) % 8)
        )

    def gather1():
        return remote(g1.at[core, me1], g1.at[core, me1], s1.at[1], t1.at[1], chip_at(base1 + 1 - me1))

    for k in range(1, 4):
        gather3(k).start()

    gather1().start()

    @pl.loop(1, 8)
    def _(k):
        gather2(k).start()


    for k in range(1, 4):
        gather3(k).wait()
    for k in range(1, 8):
        gather4(k).start()

    loads[3].wait()
    send_d = remote(d_ref, doth, one_send.at[0], one_recv.at[0], across)
    send_d.start()

    loads[2].wait()
    pt_s[...] = (iota((ROWS, ROWS), 0) == token_of(iota((ROWS, ROWS), 1), g)).astype(F32).astype(BF16)
    qa, qb, _ = levels_of(q_ref[...])
    qx1[...] = stacked(qa, 128)
    qx2[...] = stacked(qb, 32)
    kt_s[...] = tn(k_ref[...], pt_s[...]).astype(BF16)
    qt_s[...] = tn(q_ref[...], pt_s[...]).astype(BF16)
    vt_s[...] = tn(v_ref[...], pt_s[...]).astype(BF16)

    loads[5].wait()
    start1 = len_ref[0]
    start2 = start1 + len_ref[1]
    start3 = start2 + len_ref[2]

    def ids_of(pos):
        return (
            (pos >= start1).astype(jnp.int32)
            + (pos >= start2).astype(jnp.int32)
            + (pos >= start3).astype(jnp.int32)
        )

    here = seq * ROWS
    id_k = ids_of(here + token_of(iota((ROWS, 1), 0), g))
    id_q = ids_of(here + token_of(iota((1, ROWS), 1), g))

    def head_rows(i):
        return pl.ds(pl.multiple_of(i * HEAD, 16), HEAD)

    def head_forward(i):
        rows = head_rows(i)
        s = tn(kt_s[rows, :], qt_s[rows, :])
        s = jnp.where(id_k == id_q, s, NEG)
        top = jnp.max(s, axis=0, keepdims=True)
        p = jnp.exp2((s - top) * C2)
        total = jnp.sum(p, axis=0, keepdims=True)
        m0[pl.ds(i, 1), :] = top
        lse_s[pl.ds(i, 1), :] = top * C2 + jnp.log2(total)
        pb = p.astype(BF16)
        p0s[i] = pb
        a0[rows, :] = nn(vt_s[rows, :], pb) / total

    pl.loop(0, 4, unroll=2)(head_forward)

    loads[4].wait()
    own = pl.ds(pl.multiple_of(g * WIDE, 128), WIDE)
    other = pl.ds(pl.multiple_of((1 - g) * WIDE, 128), WIDE)
    base_k[...] = nt(d_ref[...], w_ref[:, own])

    gather1().wait()
    core1 = remote(g1.at[core], g1.at[core], s1.at[0], t1.at[0], partner)
    core1.start()
    pl.loop(4, HEADS, unroll=2)(head_forward)
    for k in range(1, 8):
        gather4(k).wait()
    core3 = remote(g3.at[core], g3.at[core], s3.at[0], t3.at[0], partner)
    core3.start()

    def slide_range(pos):
        lo = jnp.where(pos >= start1, start1, 0)
        lo = jnp.where(pos >= start2, start2, lo)
        lo = jnp.where(pos >= start3, start3, lo)
        hi = jnp.where(pos < start3, start3, TOKENS)
        hi = jnp.where(pos < start2, start2, hi)
        hi = jnp.where(pos < start1, start1, hi)
        return lo, hi

    def masked(s, key_pos, lo, hi):
        return jnp.where((key_pos >= lo) & (key_pos < hi), s, NEG)

    core1.wait()
    row = iota((512, 1), 0)
    kg1[...] = g1[:, :, 0:128].reshape(512, WIDE)
    vg1[...] = g1[:, :, 128:256].reshape(512, WIDE)
    colb = iota((1, 1024), 1)
    offb = (colb >> 7) & 3

    def spread1(j):
        return 4 * ((((j >> 5) & 3) + 2 * g) & 3) + 16 * ((j >> 3) & 3) + 64 * (j & 7)

    lo1, hi1 = slide_range(here + offb + spread1(colb & 127))
    lo1, hi1 = lo1 - offb, hi1 - offb
    pos1 = 512 * (2 * (base1 + ((row >> 7) & 1)) + (row >> 8)) + spread1(row & 127)
    top1, sum1, acc1 = [], [], []
    for half in range(2):
        c = slice(512 * half, 512 * half + 512)
        w = slice(128 * half, 128 * half + 256)
        sc = masked(nt(kg1[:, w], qx1[c, w]), pos1, lo1[:, c], hi1[:, c])
        top1.append(jnp.max(sc, axis=0, keepdims=True))
        pc = jnp.exp2((sc - top1[half]) * C2)
        sum1.append(jnp.sum(pc, axis=0, keepdims=True))
        p1s[:, c] = pc.astype(BF16)
        m1s[:, c] = jnp.broadcast_to(top1[half], (8, 512))
        acc1.append(tn(vg1[:, w], p1s[:, c]))

    @pl.loop(1, 8)
    def _(k):
        gather2(k).wait()

    core2 = remote(g2.at[core], g2.at[core], s2.at[0], t2.at[0], partner)
    core2.start()

    core3.wait()
    core2.wait()
    three = g3[...].astype(F32).reshape(64, 16, WIDE)
    kg23[0:512] = g2[:, :, 0:32].reshape(512, WIDE)
    vg23[0:512] = g2[:, :, 32:64].reshape(512, WIDE)
    kg23[512:1024] = three[:, 0:8].reshape(512, WIDE).astype(BF16)
    vg23[512:1024] = three[:, 8:16].reshape(512, WIDE).astype(BF16)

    col = iota((1, 256), 1)
    inner = col & 31
    off = 8 * g + (col >> 5)
    lo, hi = slide_range(here + off + 16 * (inner >> 3) + 64 * (inner & 7))
    lo, hi = lo - off, hi - off
    pos2 = 512 * (2 * (base2 + ((row >> 5) & 7)) + (row >> 8)) + 16 * ((row >> 3) & 3) + 64 * (row & 7)
    pos3 = 512 * (2 * ((row >> 3) & 31) + (row >> 8)) + 64 * (row & 7)
    sa = masked(nt(kg23[0:512], qx2[...]), pos2, lo, hi)
    sb = masked(nt(kg23[512:1024], qx2[...]), pos3, jnp.where(inner < 8, lo, FAR), hi)
    top23 = jnp.maximum(jnp.max(sa, axis=0, keepdims=True), jnp.max(sb, axis=0, keepdims=True))
    pa = jnp.exp2((sa - top23) * C2)
    pb3 = jnp.exp2((sb - top23) * C2)
    sum23 = jnp.sum(pa, axis=0, keepdims=True) + jnp.sum(pb3, axis=0, keepdims=True)
    p23s[0:512] = pa.astype(BF16)
    p23s[512:1024] = pb3.astype(BF16)
    m23s[...] = jnp.broadcast_to(top23, (8, 256))
    acc23 = tn(vg23[...], p23s[...])

    st23 = jnp.broadcast_to(top23, (8, 256))
    su23 = jnp.broadcast_to(sum23, (8, 256))
    lane8 = iota((8, 128), 1) >> 5
    lane48 = iota((HEAD, 128), 1) >> 5
    for i in range(HEADS):
        r = slice(HEAD * i, HEAD * i + HEAD)
        c = slice(128 * (i % 4), 128 * (i % 4) + 128)
        half = i // 4
        rr = slice(HEAD * i - 128 * half, HEAD * i - 128 * half + HEAD)
        two = jnp.where(lane8 == i // 4, to_tile(st23, i), NEG)[0:1]
        two_sum = jnp.where(lane8 == i // 4, to_tile(su23, i), 0.0)[0:1]
        two_acc = jnp.where(lane48 == i // 4, to_tile(acc23[r], i), 0.0)
        zero = lse_s[i : i + 1, c]
        one = top1[half][:, c] * C2
        two = two * C2
        new = jnp.maximum(jnp.maximum(zero, one), two)
        f0 = jnp.exp2(zero - new)
        f1 = jnp.exp2(one - new)
        f2 = jnp.exp2(two - new)
        l_new = f0 + sum1[half][:, c] * f1 + two_sum * f2
        a_new = (a0[r, c] * f0 + acc1[half][rr, c] * f1 + two_acc * f2) / l_new
        a0[r, c] = a_new
        lse_s[i : i + 1, c] = new + jnp.log2(l_new)

    att_t = a0[...].astype(BF16)
    att = nt(pt_s[...], att_t).astype(BF16)
    att_s[...] = att
    po_send[...] = nn(att, w_ref[:, other]).astype(BF16)

    def send_o(part):
        rows = pl.ds(256 * part, 256)
        n = 1 + part
        return remote(po_send.at[rows], po_recv.at[rows], one_send.at[n], one_recv.at[n], across)

    send_o(0).start()
    send_o(1).start()

    send_d.wait()
    for part, block in ((g, d_ref), (1 - g, doth)):
        term = tn(block[...], att)
        for c in range(16):
            x4[0, c % 4, 4 * part + c // 4] = term[24 * c : 24 * c + 16].astype(BF16)
            x4[1, c % 4, 4 * part + c // 4] = term[24 * c + 8 : 24 * c + 24].astype(BF16)
    swap4 = remote(x4.at[1 - core], y4, u4.at[0], w4.at[0], partner)
    swap4.start()
    d_att = (base_k[...] + nt(doth[...], w_ref[:, other])).astype(BF16)
    dt = tn(d_att, pt_s[...])
    dt_s[...] = dt.astype(BF16)
    da, db, _ = levels_of(d_att)
    dx1[...] = stacked(da, 128)
    dx2[...] = stacked(db, 32)

    prod = dt_s[...].astype(F32) * att_t.astype(F32)
    for i in range(HEADS):
        del_s[i : i + 1, :] = jnp.sum(prod[HEAD * i : HEAD * i + HEAD], axis=0, keepdims=True)

    swap4.wait()
    z4[...] = (x4[core].astype(F32) + y4[...].astype(F32)).astype(BF16)
    r4[z] = z4[z]

    def reduce4(k):
        return remote(z4.at[(z + k) % 4], r4.at[z], u4.at[k], w4.at[k], in_row(k))

    def reduce6(k):
        to = other_row(k)
        return remote(q4.at[to], r6.at[zrow], u4.at[8 + k], w4.at[8 + k], chip_at(4 * to + z))

    for k in range(1, 4):
        reduce4(k).start()

    def tiles_of(ref):
        return [
            jnp.broadcast_to(ref[i : i + 1, 128 * (i % 4) : 128 * (i % 4) + 128], (8, 128))
            for i in range(HEADS)
        ]

    lse_tiles, del_tiles = tiles_of(lse_s), tiles_of(del_s)
    lse23 = from_tiles(lse_tiles)[0:1]
    del23 = from_tiles(del_tiles)[0:1]
    p = p23s[...].astype(F32) * jnp.exp2(m23s[0:1] * C2 - lse23)
    ds = (p * (nt(vg23[...], dx2[...]) - del23)).astype(BF16)
    dk23 = nn(ds, qx2[...])
    dv23 = nn(p.astype(BF16), dx2[...])
    dq23 = tn(kg23[...], ds)
    x2[:, :, 0:32] = dk23[0:512].reshape(2, 8, 32, WIDE).astype(BF16)
    x2[:, :, 32:64] = dv23[0:512].reshape(2, 8, 32, WIDE).astype(BF16)
    x3[...] = jnp.concatenate(
        [dk23[512:1024].reshape(2, 32, 8, WIDE), dv23[512:1024].reshape(2, 32, 8, WIDE)], axis=2
    ).astype(BF16)
    swap3 = remote(x3.at[1 - core], y3, u3.at[0], w3.at[0], partner)
    swap3.start()
    swap2 = remote(x2.at[1 - core], y2, u2.at[0], w2.at[0], partner)
    swap2.start()

    lse1 = jnp.concatenate([t[0:1] for t in lse_tiles], axis=1)
    del1 = jnp.concatenate([t[0:1] for t in del_tiles], axis=1)
    def reduce3(k):
        to = other_row(k)
        return remote(
            z3.at[pl.ds(4 * to, 4)], r3.at[zrow], u3.at[k], w3.at[k], chip_at(4 * to + z)
        )

    def reduce5(k):
        return remote(q3.at[(z + k) % 4], r5.at[z], u3.at[8 + k], w3.at[8 + k], in_row(k))

    def reduce2(k):
        to = (me2 + k) % 8
        return remote(z2.at[to], r2.at[me2], u2.at[k], w2.at[k], chip_at(base2 + to))

    def reduce1():
        return remote(z1.at[1 - me1], r1.at[me1], u1.at[1], w1.at[1], chip_at(base1 + 1 - me1))

    def send_third():
        swap3.wait()
        z3[...] = (x3[core].astype(F32) + y3[...].astype(F32)).astype(BF16)
        r3[zrow] = z3[pl.ds(4 * zrow, 4)]
        for k in range(1, 8):
            reduce3(k).start()

    dk1, dv1, dq1 = [], [], []
    for half in range(2):
        if half == 1:
            send_third()
        c = slice(512 * half, 512 * half + 512)
        w = slice(128 * half, 128 * half + 256)
        p = p1s[:, c].astype(F32) * jnp.exp2(m1s[0:1, c] * C2 - lse1[:, c])
        ds = (p * (nt(vg1[:, w], dx1[c, w]) - del1[:, c])).astype(BF16)
        dk1.append(nn(ds, qx1[c, w]))
        dv1.append(nn(p.astype(BF16), dx1[c, w]))
        dq1.append(tn(kg1[:, w], ds))

    def joined(a, b):
        return jnp.concatenate([a[:, 0:128], a[:, 128:256] + b[:, 0:128], b[:, 128:256]], axis=1)

    dk1, dv1 = joined(*dk1), joined(*dv1)
    x1[:, :, 0:128] = dk1.reshape(2, 2, 128, WIDE).astype(BF16)
    x1[:, :, 128:256] = dv1.reshape(2, 2, 128, WIDE).astype(BF16)
    swap1 = remote(x1.at[1 - core], y1, u1.at[0], w1.at[0], partner)
    swap1.start()

    swap2.wait()
    z2[...] = (x2[core].astype(F32) + y2[...].astype(F32)).astype(BF16)
    r2[me2] = z2[me2]

    @pl.loop(1, 8)
    def _(k):
        reduce2(k).start()

    a0[...] = jnp.concatenate(
        [jnp.exp2(m0[...] * C2 - lse_s[...])] * (WIDE // HEADS), axis=0
    )

    def head_back(i):
        rows = head_rows(i)
        p = p0s[i].astype(F32) * a0[pl.ds(i, 1), :]
        pb = p.astype(BF16)
        dp = tn(vt_s[rows, :], dt_s[rows, :])
        ds = (p * (dp - del_s[pl.ds(i, 1), :])).astype(BF16)
        dqt[rows, :] = nn(kt_s[rows, :], ds)
        dkt[rows, :] = nt(qt_s[rows, :], ds)
        dvt[rows, :] = nt(dt_s[rows, :], pb)

    pl.loop(0, 2, unroll=2)(head_back)
    swap1.wait()
    z1[...] = (x1[core].astype(F32) + y1[...].astype(F32)).astype(BF16)
    r1[me1] = z1[me1]
    reduce1().start()
    for k in range(1, 4):
        reduce4(k).wait()
    q4[...] = jnp.sum(r4[...].astype(F32), axis=0).astype(BF16)
    r6[zrow] = q4[zrow]
    for k in range(1, 8):
        reduce6(k).start()
    pl.loop(2, 4, unroll=2)(head_back)
    for k in range(1, 8):
        reduce3(k).wait()
    q3[...] = jnp.sum(r3[...].astype(F32), axis=0).astype(BF16)
    r5[z] = q3[z]
    for k in range(1, 4):
        reduce5(k).start()
    pl.loop(4, 8, unroll=4)(head_back)

    for i in range(HEADS):
        r = slice(HEAD * i, HEAD * i + HEAD)
        c = slice(128 * (i % 4), 128 * (i % 4) + 128)
        half = i // 4
        rr = slice(HEAD * i - 128 * half, HEAD * i - 128 * half + HEAD)
        two = jnp.where(lane48 == half, to_tile(dq23[r], i), 0.0)
        dqt[r, c] = dqt[r, c] + dq1[half][rr, c] + two
    dq_ref[...] = nt(pt_s[...], (dqt[...] * SCALE).astype(BF16)).astype(BF16)

    for level0, scale, kept in ((dkt, SCALE, base_k), (dvt, 1.0, base_v)):
        kept[...] = nt(pt_s[...], (level0[...] * scale).astype(BF16))

    for k in range(1, 8):
        reduce6(k).wait()
    four = jnp.sum(r6[...].astype(F32), axis=0) * (TOKENS**-0.5)
    dw_ref[...] = jnp.where(core == 0, four, pltpu.roll(four, 12, 0))

    @pl.loop(1, 8)
    def _(k):
        reduce2(k).wait()

    two = jnp.sum(r2[...].astype(F32), axis=0)
    send_o(0).wait()
    send_o(1).wait()
    out_ref[...] = (nn(att_s[...], w_ref[:, own]) + po_recv[...].astype(F32)).astype(BF16)
    for k in range(1, 4):
        reduce5(k).wait()
    three = jnp.sum(r5[...].astype(F32), axis=0)
    reduce1().wait()
    one = jnp.sum(r1[...].astype(F32), axis=0)
    low = iota((32, WIDE), 1) < 4 * HEAD
    cls = lane_head(128) & 3

    def whole(first, second, third, kept, scale):
        second = jnp.concatenate([second[0:8] + third, second[8:32]], axis=0)
        first = jnp.concatenate(
            [
                first[0:32] + jnp.where(low, second, 0.0),
                first[32:64] + jnp.where(low, 0.0, second),
                first[64:128],
            ],
            axis=0,
        )
        first = first * scale
        full = jnp.concatenate([jnp.where(cls == j, first, 0.0) for j in range(4)], axis=0)
        return (nn(pt_s[...], full.astype(BF16)) + kept[...]).astype(BF16)

    dk_ref[...] = whole(one[0:128], two[0:32], three[0:8], base_k, SCALE)
    dv_ref[...] = whole(one[128:256], two[32:64], three[8:16], base_v, 1.0)


def finish(a, b, c, d, e, out, dq, dk, dv, dw, sem):
    moves = [
        pltpu.make_async_copy(given, result, sem.at[n])
        for n, (given, result) in enumerate(((a, out), (b, dq), (c, dk), (d, dv)))
    ]
    for move in moves:
        move.start()
    dw[...] = e[0:12]
    for move in moves:
        move.wait()


def shards(queries, keys, values, w_out, d_out, slide_lengths):
    vmem = pl.BlockSpec(memory_space=pltpu.VMEM)
    anywhere = pl.BlockSpec(memory_space=pl.ANY)
    shape = jax.ShapeDtypeStruct

    def v(*dims, dtype=BF16):
        return pltpu.VMEM(dims, dtype)

    def sems(n):
        return pltpu.SemaphoreType.DMA((n,))

    scratch = [
        v(512, WIDE), v(512, WIDE), v(512, WIDE), v(WIDE, 768), v(512, WIDE),
        pltpu.SMEM((4,), jnp.int32), sems(6),
        v(512, 512), v(512, 512),
        v(WIDE, 512), v(WIDE, 512), v(WIDE, 512), v(WIDE, 512),
        v(1024, WIDE), v(256, WIDE), v(1024, WIDE), v(256, WIDE),
        v(2, 2, 256, WIDE), v(2, 8, 64, WIDE), v(2, 32, 16, WIDE),
        v(1024, WIDE), v(1024, WIDE), v(512, WIDE), v(512, WIDE),
        v(8, 512, 512), v(512, 1024), v(1024, 256),
        v(WIDE, 512, dtype=F32), v(8, 512, dtype=F32),
        v(8, 512, dtype=F32), v(8, 512, dtype=F32), v(8, 1024, dtype=F32), v(8, 256, dtype=F32),
        v(WIDE, 512, dtype=F32), v(WIDE, 512, dtype=F32), v(WIDE, 512, dtype=F32),
        v(512, WIDE, dtype=F32), v(512, WIDE, dtype=F32),
        v(512, WIDE), v(512, WIDE), v(512, WIDE), v(512, WIDE),
        v(2, 2, 256, WIDE), v(2, 8, 64, WIDE), v(2, 32, 16, WIDE), v(2, 4, 8, 16, WIDE),
        v(2, 256, WIDE), v(8, 64, WIDE), v(32, 16, WIDE), v(4, 8, 16, WIDE),
        v(2, 256, WIDE), v(8, 64, WIDE), v(32, 16, WIDE), v(4, 8, 16, WIDE),
        v(2, 256, WIDE), v(8, 64, WIDE), v(8, 4, 16, WIDE), v(4, 8, 16, WIDE),
        v(4, 16, WIDE), v(8, 16, WIDE), v(4, 16, WIDE), v(8, 16, WIDE),
        sems(3), sems(3),
        sems(2), sems(2), sems(8), sems(8), sems(32), sems(32),
        sems(2), sems(2), sems(8), sems(8), sems(32), sems(32), sems(32), sems(32),
    ]
    out, dq, dk, dv, dw = pl.pallas_call(
        kernel,
        out_shape=[shape((ROWS, WIDE), BF16)] * 4 + [shape((16, WIDE), F32)],
        in_specs=[anywhere] * 6,
        out_specs=[vmem] * 5,
        scratch_shapes=scratch,
        compiler_params=pltpu.CompilerParams(
            collective_id=0, has_side_effects=True, vmem_limit_bytes=54_800_000
        ),
    )(queries, keys, values, w_out, d_out, slide_lengths)
    out, dq, dk, dv, dw = pl.pallas_call(
        finish,
        out_shape=[shape((ROWS, WIDE), BF16)] * 4 + [shape((12, WIDE), F32)],
        in_specs=[anywhere] * 4 + [vmem],
        out_specs=[anywhere] * 4 + [vmem],
        scratch_shapes=[sems(4)],
        compiler_params=pltpu.CompilerParams(vmem_limit_bytes=4 * 1024 * 1024),
    )(out, dq, dk, dv, dw)
    return out, dq, dk, dv, dw.T


def solution(mesh):
    both = P("seq", "head")
    return jax.shard_map(
        shards,
        mesh=mesh,
        in_specs=(both, both, both, P("head", None), both, P()),
        out_specs=(both, both, both, both, P("head", "seq")),
        check_vma=False,
    )
```

```python
import jax
import jax.numpy as jnp
from jax import lax
from jax.experimental import pallas as pl
from jax.experimental.pallas import tpu as pltpu
from jax.sharding import PartitionSpec as P

TOKENS = 32768
HEAD = 48
ROWS = 512
WIDE = 384
HEADS = 8
NEG = -1e30
SCALE = HEAD**-0.5
LOG2E = 1.4426950408889634
C2 = SCALE * LOG2E
FAR = 1 << 30
F32 = jnp.float32
BF16 = jnp.bfloat16
MESH = pl.DeviceIdType.MESH


def nn(a, b):
    return lax.dot_general(a, b, (((1,), (0,)), ((), ())), preferred_element_type=F32)


def nt(a, b):
    return lax.dot_general(a, b, (((1,), (1,)), ((), ())), preferred_element_type=F32)


def tn(a, b):
    return lax.dot_general(a, b, (((0,), (0,)), ((), ())), preferred_element_type=F32)


def iota(shape, dim):
    return lax.broadcasted_iota(jnp.int32, shape, dim)


def token_of(a, g):
    return (a >> 7) + 4 * ((((a >> 5) & 3) + 2 * g) & 3) + 16 * ((a >> 3) & 3) + 64 * (a & 7)


def lane_head(rows):
    lane = iota((rows, WIDE), 1)
    head = jnp.zeros_like(lane)
    for i in range(1, HEADS):
        head = head + (lane >= HEAD * i).astype(jnp.int32)
    return head


def compact1(x):
    cls = lane_head(128) & 3
    y = jnp.where(cls == 0, x[0:128], x[128:256])
    y = jnp.where(cls == 2, x[256:384], y)
    return jnp.where(cls == 3, x[384:512], y)


def compact2(x1):
    return jnp.where(iota((32, WIDE), 1) < 4 * HEAD, x1[0:32], x1[32:64])


def stacked(x, n):
    rows = HEADS * n
    shift = n.bit_length() - 1
    own = (iota((rows, WIDE), 0) >> shift) == lane_head(rows)
    return jnp.where(own, jnp.concatenate([x] * HEADS, axis=0), 0.0).astype(BF16)


def to_tile(x, i):
    t, at, to = i // 4, 32 * (i % 4), 32 * (i // 4)
    tile = x[:, 128 * t : 128 * t + 128]
    shift = (to - at) % 128
    return pltpu.roll(tile, shift, 1) if shift else tile


def from_tiles(tiles):
    halves = []
    for t in range(2):
        lane = iota(tiles[0].shape, 1)
        half = None
        for i in range(4 * t, 4 * t + 4):
            at, to = 32 * (i % 4), 32 * (i // 4)
            shift = (at - to) % 128
            moved = pltpu.roll(tiles[i], shift, 1) if shift else tiles[i]
            half = moved if half is None else jnp.where((lane >> 5) == (i % 4), moved, half)
        halves.append(half)
    return jnp.concatenate(halves, axis=1)


def kernel(
    q_in, k_in, v_in, w_in, d_in, len_in,
    out_ref, dq_ref, dk_ref, dv_ref, dw_ref,
    q_ref, k_ref, v_ref, w_ref, d_ref, len_ref, in_sem,
    p_s, pt_s, qt_s, kt_s, vt_s, dt_s, qx1, qx2, dx1, dx2,
    g1, g2, g3, kg23, vg23, kg1, vg1, p0s, p1s, p23s,
    a0, m0, lse_s, del_s, m1s, m23s, dqt, dkt, dvt, base_k, base_v,
    doth, att_s, po_send, po_recv,
    x1, x2, x3, x4, y1, y2, y3, y4, z1, z2, z3, z4, r1, r2, r3, r4, q3, q4, r5, r6,
    one_send, one_recv, s1, t1, s2, t2, s3, t3, u1, w1, u2, w2, u3, w3, u4, w4,
):
    seq = lax.axis_index("seq")
    g = lax.axis_index("head")
    chip = seq // 2
    core = seq % 2
    partner = {"seq": chip * 2 + (1 - core), "head": g}
    across = {"seq": seq, "head": 1 - g}

    def chip_at(c):
        return {"seq": c * 2 + core, "head": g}

    base1, base2 = (chip // 2) * 2, (chip // 8) * 8
    me1, me2, me3 = chip - base1, chip - base2, chip
    z, zrow = chip % 4, chip // 4
    row_low = zrow + 1 - 2 * (zrow % 2)

    def in_row(k):
        return chip_at(4 * zrow + (z + k) % 4)

    def other_row(k):
        return (zrow + k) % 8

    loads = [
        pltpu.make_async_copy(a, b, in_sem.at[n])
        for n, (a, b) in enumerate(
            ((k_in, k_ref), (v_in, v_ref), (q_in, q_ref), (d_in, d_ref), (w_in, w_ref), (len_in, len_ref))
        )
    ]
    loads[0].start()
    loads[1].start()
    barrier = pltpu.get_barrier_semaphore()
    pl.semaphore_signal(barrier, inc=1, device_id=partner, device_id_type=MESH)
    pl.semaphore_signal(barrier, inc=1, device_id=across, device_id_type=MESH)

    for k in range(1, 4):
        pl.semaphore_signal(barrier, inc=1, device_id=in_row(k), device_id_type=MESH)
        pl.semaphore_signal(
            barrier, inc=1, device_id=chip_at(4 * row_low + (z + k) % 4), device_id_type=MESH
        )
    for k in range(1, 8):
        pl.semaphore_signal(
            barrier, inc=1, device_id=chip_at(4 * other_row(k) + z), device_id_type=MESH
        )

    p_s[...] = (iota((ROWS, ROWS), 1) == token_of(iota((ROWS, ROWS), 0), g)).astype(F32).astype(BF16)

    def levels_of(x):
        y1_ = compact1(nn(p_s[...], x))
        y2_ = compact2(y1_)
        return y1_, y2_, y2_[0:8]

    loads[0].wait()
    ka, kb, kc = levels_of(k_ref[...])
    loads[1].wait()
    for n in (2, 3, 4, 5):
        loads[n].start()
    va, vb, vc = levels_of(v_ref[...])
    g1[core, me1, 0:128] = ka.astype(BF16)
    g1[core, me1, 128:256] = va.astype(BF16)
    g2[core, me2, 0:32] = kb.astype(BF16)
    g2[core, me2, 32:64] = vb.astype(BF16)
    g3[core, me3] = jnp.concatenate([kc, vc], axis=0).astype(BF16)

    pl.semaphore_wait(barrier, 15)

    def remote(src, dst, ss, rs, dev):
        return pltpu.make_async_remote_copy(
            src_ref=src, dst_ref=dst, send_sem=ss, recv_sem=rs, device_id=dev, device_id_type=MESH
        )

    def gather3(k):
        return remote(g3.at[core, me3], g3.at[core, me3], s3.at[k], t3.at[k], in_row(k))

    def gather4(k):
        row = g3.at[core, pl.ds(4 * zrow, 4)]
        return remote(row, row, s3.at[8 + k], t3.at[8 + k], chip_at(4 * other_row(k) + z))

    def gather2(k):
        return remote(
            g2.at[core, me2], g2.at[core, me2], s2.at[k], t2.at[k], chip_at(base2 + (me2 + k) % 8)
        )

    def gather1():
        return remote(g1.at[core, me1], g1.at[core, me1], s1.at[1], t1.at[1], chip_at(base1 + 1 - me1))

    for k in range(1, 4):
        gather3(k).start()

    gather1().start()

    @pl.loop(1, 8)
    def _(k):
        gather2(k).start()


    loads[2].wait()
    pt_s[...] = (iota((ROWS, ROWS), 0) == token_of(iota((ROWS, ROWS), 1), g)).astype(F32).astype(BF16)
    qa, qb, _ = levels_of(q_ref[...])
    for k in range(1, 4):
        gather3(k).wait()
    for k in range(1, 8):
        gather4(k).start()

    loads[3].wait()
    send_d = remote(d_ref, doth, one_send.at[0], one_recv.at[0], across)
    send_d.start()

    qx1[...] = stacked(qa, 128)
    qx2[...] = stacked(qb, 32)
    kt_s[...] = tn(k_ref[...], pt_s[...]).astype(BF16)
    qt_s[...] = tn(q_ref[...], pt_s[...]).astype(BF16)
    vt_s[...] = tn(v_ref[...], pt_s[...]).astype(BF16)

    loads[5].wait()
    start1 = len_ref[0]
    start2 = start1 + len_ref[1]
    start3 = start2 + len_ref[2]

    def ids_of(pos):
        return (
            (pos >= start1).astype(jnp.int32)
            + (pos >= start2).astype(jnp.int32)
            + (pos >= start3).astype(jnp.int32)
        )

    here = seq * ROWS
    id_k = ids_of(here + token_of(iota((ROWS, 1), 0), g))
    id_q = ids_of(here + token_of(iota((1, ROWS), 1), g))

    def head_rows(i):
        return pl.ds(pl.multiple_of(i * HEAD, 16), HEAD)

    def head_forward(i):
        rows = head_rows(i)
        s = tn(kt_s[rows, :], qt_s[rows, :])
        s = jnp.where(id_k == id_q, s, NEG)
        top = jnp.max(s, axis=0, keepdims=True)
        p = jnp.exp2((s - top) * C2)
        total = jnp.sum(p, axis=0, keepdims=True)
        m0[pl.ds(i, 1), :] = top
        lse_s[pl.ds(i, 1), :] = top * C2 + jnp.log2(total)
        pb = p.astype(BF16)
        p0s[i] = pb
        a0[rows, :] = nn(vt_s[rows, :], pb) / total

    pl.loop(0, 4, unroll=2)(head_forward)

    loads[4].wait()
    own = pl.ds(pl.multiple_of(g * WIDE, 128), WIDE)
    other = pl.ds(pl.multiple_of((1 - g) * WIDE, 128), WIDE)
    base_k[...] = nt(d_ref[...], w_ref[:, own])

    gather1().wait()
    core1 = remote(g1.at[core], g1.at[core], s1.at[0], t1.at[0], partner)
    core1.start()
    pl.loop(4, HEADS, unroll=2)(head_forward)
    for k in range(1, 8):
        gather4(k).wait()
    core3 = remote(g3.at[core], g3.at[core], s3.at[0], t3.at[0], partner)
    core3.start()

    def slide_range(pos):
        lo = jnp.where(pos >= start1, start1, 0)
        lo = jnp.where(pos >= start2, start2, lo)
        lo = jnp.where(pos >= start3, start3, lo)
        hi = jnp.where(pos < start3, start3, TOKENS)
        hi = jnp.where(pos < start2, start2, hi)
        hi = jnp.where(pos < start1, start1, hi)
        return lo, hi

    def masked(s, key_pos, lo, hi):
        return jnp.where((key_pos >= lo) & (key_pos < hi), s, NEG)

    core1.wait()
    row = iota((512, 1), 0)
    kg1[...] = g1[:, :, 0:128].reshape(512, WIDE)
    vg1[...] = g1[:, :, 128:256].reshape(512, WIDE)
    colb = iota((1, 1024), 1)
    offb = (colb >> 7) & 3

    def spread1(j):
        return 4 * ((((j >> 5) & 3) + 2 * g) & 3) + 16 * ((j >> 3) & 3) + 64 * (j & 7)

    lo1, hi1 = slide_range(here + offb + spread1(colb & 127))
    lo1, hi1 = lo1 - offb, hi1 - offb
    pos1 = 512 * (2 * (base1 + ((row >> 7) & 1)) + (row >> 8)) + spread1(row & 127)
    top1, sum1, acc1 = [], [], []
    for half in range(2):
        c = slice(512 * half, 512 * half + 512)
        w = slice(128 * half, 128 * half + 256)
        sc = masked(nt(kg1[:, w], qx1[c, w]), pos1, lo1[:, c], hi1[:, c])
        top1.append(jnp.max(sc, axis=0, keepdims=True))
        pc = jnp.exp2((sc - top1[half]) * C2)
        sum1.append(jnp.sum(pc, axis=0, keepdims=True))
        p1s[:, c] = pc.astype(BF16)
        m1s[:, c] = jnp.broadcast_to(top1[half], (8, 512))
        acc1.append(tn(vg1[:, w], p1s[:, c]))

    @pl.loop(1, 8)
    def _(k):
        gather2(k).wait()

    core2 = remote(g2.at[core], g2.at[core], s2.at[0], t2.at[0], partner)
    core2.start()

    core3.wait()
    core2.wait()
    three = g3[...].astype(F32).reshape(64, 16, WIDE)
    kg23[0:512] = g2[:, :, 0:32].reshape(512, WIDE)
    vg23[0:512] = g2[:, :, 32:64].reshape(512, WIDE)
    kg23[512:1024] = three[:, 0:8].reshape(512, WIDE).astype(BF16)
    vg23[512:1024] = three[:, 8:16].reshape(512, WIDE).astype(BF16)

    col = iota((1, 256), 1)
    inner = col & 31
    off = 8 * g + (col >> 5)
    lo, hi = slide_range(here + off + 16 * (inner >> 3) + 64 * (inner & 7))
    lo, hi = lo - off, hi - off
    pos2 = 512 * (2 * (base2 + ((row >> 5) & 7)) + (row >> 8)) + 16 * ((row >> 3) & 3) + 64 * (row & 7)
    pos3 = 512 * (2 * ((row >> 3) & 31) + (row >> 8)) + 64 * (row & 7)
    sa = masked(nt(kg23[0:512], qx2[...]), pos2, lo, hi)
    sb = masked(nt(kg23[512:1024], qx2[...]), pos3, jnp.where(inner < 8, lo, FAR), hi)
    top23 = jnp.maximum(jnp.max(sa, axis=0, keepdims=True), jnp.max(sb, axis=0, keepdims=True))
    pa = jnp.exp2((sa - top23) * C2)
    pb3 = jnp.exp2((sb - top23) * C2)
    sum23 = jnp.sum(pa, axis=0, keepdims=True) + jnp.sum(pb3, axis=0, keepdims=True)
    p23s[0:512] = pa.astype(BF16)
    p23s[512:1024] = pb3.astype(BF16)
    m23s[...] = jnp.broadcast_to(top23, (8, 256))
    acc23 = tn(vg23[...], p23s[...])

    st23 = jnp.broadcast_to(top23, (8, 256))
    su23 = jnp.broadcast_to(sum23, (8, 256))
    lane8 = iota((8, 128), 1) >> 5
    lane48 = iota((HEAD, 128), 1) >> 5
    for i in range(HEADS):
        r = slice(HEAD * i, HEAD * i + HEAD)
        c = slice(128 * (i % 4), 128 * (i % 4) + 128)
        half = i // 4
        rr = slice(HEAD * i - 128 * half, HEAD * i - 128 * half + HEAD)
        two = jnp.where(lane8 == i // 4, to_tile(st23, i), NEG)[0:1]
        two_sum = jnp.where(lane8 == i // 4, to_tile(su23, i), 0.0)[0:1]
        two_acc = jnp.where(lane48 == i // 4, to_tile(acc23[r], i), 0.0)
        zero = lse_s[i : i + 1, c]
        one = top1[half][:, c] * C2
        two = two * C2
        new = jnp.maximum(jnp.maximum(zero, one), two)
        f0 = jnp.exp2(zero - new)
        f1 = jnp.exp2(one - new)
        f2 = jnp.exp2(two - new)
        l_new = f0 + sum1[half][:, c] * f1 + two_sum * f2
        a_new = (a0[r, c] * f0 + acc1[half][rr, c] * f1 + two_acc * f2) / l_new
        a0[r, c] = a_new
        lse_s[i : i + 1, c] = new + jnp.log2(l_new)

    att_t = a0[...].astype(BF16)
    att = nt(pt_s[...], att_t).astype(BF16)
    att_s[...] = att
    po_send[...] = nn(att, w_ref[:, other]).astype(BF16)

    def send_o(part):
        rows = pl.ds(256 * part, 256)
        n = 1 + part
        return remote(po_send.at[rows], po_recv.at[rows], one_send.at[n], one_recv.at[n], across)

    send_o(0).start()
    send_o(1).start()

    send_d.wait()
    for part, block in ((g, d_ref), (1 - g, doth)):
        term = tn(block[...], att)
        for c in range(16):
            x4[0, c % 4, 4 * part + c // 4] = term[24 * c : 24 * c + 16].astype(BF16)
            x4[1, c % 4, 4 * part + c // 4] = term[24 * c + 8 : 24 * c + 24].astype(BF16)
    swap4 = remote(x4.at[1 - core], y4, u4.at[0], w4.at[0], partner)
    swap4.start()
    d_att = (base_k[...] + nt(doth[...], w_ref[:, other])).astype(BF16)
    dt = tn(d_att, pt_s[...])
    dt_s[...] = dt.astype(BF16)
    da, db, _ = levels_of(d_att)
    dx1[...] = stacked(da, 128)
    dx2[...] = stacked(db, 32)

    prod = dt_s[...].astype(F32) * att_t.astype(F32)
    for i in range(HEADS):
        del_s[i : i + 1, :] = jnp.sum(prod[HEAD * i : HEAD * i + HEAD], axis=0, keepdims=True)

    swap4.wait()
    z4[...] = (x4[core].astype(F32) + y4[...].astype(F32)).astype(BF16)
    r4[z] = z4[z]

    def reduce4(k):
        return remote(z4.at[(z + k) % 4], r4.at[z], u4.at[k], w4.at[k], in_row(k))

    def reduce6(k):
        to = other_row(k)
        return remote(q4.at[to], r6.at[zrow], u4.at[8 + k], w4.at[8 + k], chip_at(4 * to + z))

    for k in range(1, 4):
        reduce4(k).start()

    def tiles_of(ref):
        return [
            jnp.broadcast_to(ref[i : i + 1, 128 * (i % 4) : 128 * (i % 4) + 128], (8, 128))
            for i in range(HEADS)
        ]

    lse_tiles, del_tiles = tiles_of(lse_s), tiles_of(del_s)
    lse23 = from_tiles(lse_tiles)[0:1]
    del23 = from_tiles(del_tiles)[0:1]
    p = p23s[...].astype(F32) * jnp.exp2(m23s[0:1] * C2 - lse23)
    ds = (p * (nt(vg23[...], dx2[...]) - del23)).astype(BF16)
    dk23 = nn(ds, qx2[...])
    dv23 = nn(p.astype(BF16), dx2[...])
    dq23 = tn(kg23[...], ds)
    x2[:, :, 0:32] = dk23[0:512].reshape(2, 8, 32, WIDE).astype(BF16)
    x2[:, :, 32:64] = dv23[0:512].reshape(2, 8, 32, WIDE).astype(BF16)
    x3[...] = jnp.concatenate(
        [dk23[512:1024].reshape(2, 32, 8, WIDE), dv23[512:1024].reshape(2, 32, 8, WIDE)], axis=2
    ).astype(BF16)
    swap3 = remote(x3.at[1 - core], y3, u3.at[0], w3.at[0], partner)
    swap3.start()
    swap2 = remote(x2.at[1 - core], y2, u2.at[0], w2.at[0], partner)
    swap2.start()

    lse1 = jnp.concatenate([t[0:1] for t in lse_tiles], axis=1)
    del1 = jnp.concatenate([t[0:1] for t in del_tiles], axis=1)
    def reduce3(k):
        to = other_row(k)
        return remote(
            z3.at[pl.ds(4 * to, 4)], r3.at[zrow], u3.at[k], w3.at[k], chip_at(4 * to + z)
        )

    def reduce5(k):
        return remote(q3.at[(z + k) % 4], r5.at[z], u3.at[8 + k], w3.at[8 + k], in_row(k))

    def reduce2(k):
        to = (me2 + k) % 8
        return remote(z2.at[to], r2.at[me2], u2.at[k], w2.at[k], chip_at(base2 + to))

    def reduce1():
        return remote(z1.at[1 - me1], r1.at[me1], u1.at[1], w1.at[1], chip_at(base1 + 1 - me1))

    def send_third():
        swap3.wait()
        z3[...] = (x3[core].astype(F32) + y3[...].astype(F32)).astype(BF16)
        r3[zrow] = z3[pl.ds(4 * zrow, 4)]
        for k in range(1, 8):
            reduce3(k).start()

    dk1, dv1, dq1 = [], [], []
    for half in range(2):
        if half == 1:
            send_third()
        c = slice(512 * half, 512 * half + 512)
        w = slice(128 * half, 128 * half + 256)
        p = p1s[:, c].astype(F32) * jnp.exp2(m1s[0:1, c] * C2 - lse1[:, c])
        ds = (p * (nt(vg1[:, w], dx1[c, w]) - del1[:, c])).astype(BF16)
        dk1.append(nn(ds, qx1[c, w]))
        dv1.append(nn(p.astype(BF16), dx1[c, w]))
        dq1.append(tn(kg1[:, w], ds))

    def joined(a, b):
        return jnp.concatenate([a[:, 0:128], a[:, 128:256] + b[:, 0:128], b[:, 128:256]], axis=1)

    dk1, dv1 = joined(*dk1), joined(*dv1)
    x1[:, :, 0:128] = dk1.reshape(2, 2, 128, WIDE).astype(BF16)
    x1[:, :, 128:256] = dv1.reshape(2, 2, 128, WIDE).astype(BF16)
    swap1 = remote(x1.at[1 - core], y1, u1.at[0], w1.at[0], partner)
    swap1.start()

    swap2.wait()
    z2[...] = (x2[core].astype(F32) + y2[...].astype(F32)).astype(BF16)
    r2[me2] = z2[me2]

    @pl.loop(1, 8)
    def _(k):
        reduce2(k).start()

    a0[...] = jnp.concatenate(
        [jnp.exp2(m0[...] * C2 - lse_s[...])] * (WIDE // HEADS), axis=0
    )

    def head_back(i):
        rows = head_rows(i)
        p = p0s[i].astype(F32) * a0[pl.ds(i, 1), :]
        pb = p.astype(BF16)
        dp = tn(vt_s[rows, :], dt_s[rows, :])
        ds = (p * (dp - del_s[pl.ds(i, 1), :])).astype(BF16)
        dqt[rows, :] = nn(kt_s[rows, :], ds)
        dkt[rows, :] = nt(qt_s[rows, :], ds)
        dvt[rows, :] = nt(dt_s[rows, :], pb)

    pl.loop(0, 2, unroll=2)(head_back)
    swap1.wait()
    z1[...] = (x1[core].astype(F32) + y1[...].astype(F32)).astype(BF16)
    r1[me1] = z1[me1]
    reduce1().start()
    for k in range(1, 4):
        reduce4(k).wait()
    q4[...] = jnp.sum(r4[...].astype(F32), axis=0).astype(BF16)
    r6[zrow] = q4[zrow]
    for k in range(1, 8):
        reduce6(k).start()
    pl.loop(2, 4, unroll=2)(head_back)
    for k in range(1, 8):
        reduce3(k).wait()
    q3[...] = jnp.sum(r3[...].astype(F32), axis=0).astype(BF16)
    r5[z] = q3[z]
    for k in range(1, 4):
        reduce5(k).start()
    pl.loop(4, 8, unroll=4)(head_back)

    for i in range(HEADS):
        r = slice(HEAD * i, HEAD * i + HEAD)
        c = slice(128 * (i % 4), 128 * (i % 4) + 128)
        half = i // 4
        rr = slice(HEAD * i - 128 * half, HEAD * i - 128 * half + HEAD)
        two = jnp.where(lane48 == half, to_tile(dq23[r], i), 0.0)
        dqt[r, c] = dqt[r, c] + dq1[half][rr, c] + two
    dq_ref[...] = nt(pt_s[...], (dqt[...] * SCALE).astype(BF16)).astype(BF16)

    for level0, scale, kept in ((dkt, SCALE, base_k), (dvt, 1.0, base_v)):
        kept[...] = nt(pt_s[...], (level0[...] * scale).astype(BF16))

    for k in range(1, 8):
        reduce6(k).wait()
    four = jnp.sum(r6[...].astype(F32), axis=0) * (TOKENS**-0.5)
    dw_ref[...] = jnp.where(core == 0, four, pltpu.roll(four, 12, 0))

    @pl.loop(1, 8)
    def _(k):
        reduce2(k).wait()

    two = jnp.sum(r2[...].astype(F32), axis=0)
    send_o(0).wait()
    send_o(1).wait()
    out_ref[...] = (nn(att_s[...], w_ref[:, own]) + po_recv[...].astype(F32)).astype(BF16)
    for k in range(1, 4):
        reduce5(k).wait()
    three = jnp.sum(r5[...].astype(F32), axis=0)
    reduce1().wait()
    one = jnp.sum(r1[...].astype(F32), axis=0)
    low = iota((32, WIDE), 1) < 4 * HEAD
    cls = lane_head(128) & 3

    def whole(first, second, third, kept, scale):
        second = jnp.concatenate([second[0:8] + third, second[8:32]], axis=0)
        first = jnp.concatenate(
            [
                first[0:32] + jnp.where(low, second, 0.0),
                first[32:64] + jnp.where(low, 0.0, second),
                first[64:128],
            ],
            axis=0,
        )
        first = first * scale
        full = jnp.concatenate([jnp.where(cls == j, first, 0.0) for j in range(4)], axis=0)
        return (nn(pt_s[...], full.astype(BF16)) + kept[...]).astype(BF16)

    dk_ref[...] = whole(one[0:128], two[0:32], three[0:8], base_k, SCALE)
    dv_ref[...] = whole(one[128:256], two[32:64], three[8:16], base_v, 1.0)


def finish(a, b, c, d, e, out, dq, dk, dv, dw, sem):
    moves = [
        pltpu.make_async_copy(given, result, sem.at[n])
        for n, (given, result) in enumerate(((a, out), (b, dq), (c, dk), (d, dv)))
    ]
    for move in moves:
        move.start()
    dw[...] = e[0:12]
    for move in moves:
        move.wait()


def shards(queries, keys, values, w_out, d_out, slide_lengths):
    vmem = pl.BlockSpec(memory_space=pltpu.VMEM)
    anywhere = pl.BlockSpec(memory_space=pl.ANY)
    shape = jax.ShapeDtypeStruct

    def v(*dims, dtype=BF16):
        return pltpu.VMEM(dims, dtype)

    def sems(n):
        return pltpu.SemaphoreType.DMA((n,))

    scratch = [
        v(512, WIDE), v(512, WIDE), v(512, WIDE), v(WIDE, 768), v(512, WIDE),
        pltpu.SMEM((4,), jnp.int32), sems(6),
        v(512, 512), v(512, 512),
        v(WIDE, 512), v(WIDE, 512), v(WIDE, 512), v(WIDE, 512),
        v(1024, WIDE), v(256, WIDE), v(1024, WIDE), v(256, WIDE),
        v(2, 2, 256, WIDE), v(2, 8, 64, WIDE), v(2, 32, 16, WIDE),
        v(1024, WIDE), v(1024, WIDE), v(512, WIDE), v(512, WIDE),
        v(8, 512, 512), v(512, 1024), v(1024, 256),
        v(WIDE, 512, dtype=F32), v(8, 512, dtype=F32),
        v(8, 512, dtype=F32), v(8, 512, dtype=F32), v(8, 1024, dtype=F32), v(8, 256, dtype=F32),
        v(WIDE, 512, dtype=F32), v(WIDE, 512, dtype=F32), v(WIDE, 512, dtype=F32),
        v(512, WIDE, dtype=F32), v(512, WIDE, dtype=F32),
        v(512, WIDE), v(512, WIDE), v(512, WIDE), v(512, WIDE),
        v(2, 2, 256, WIDE), v(2, 8, 64, WIDE), v(2, 32, 16, WIDE), v(2, 4, 8, 16, WIDE),
        v(2, 256, WIDE), v(8, 64, WIDE), v(32, 16, WIDE), v(4, 8, 16, WIDE),
        v(2, 256, WIDE), v(8, 64, WIDE), v(32, 16, WIDE), v(4, 8, 16, WIDE),
        v(2, 256, WIDE), v(8, 64, WIDE), v(8, 4, 16, WIDE), v(4, 8, 16, WIDE),
        v(4, 16, WIDE), v(8, 16, WIDE), v(4, 16, WIDE), v(8, 16, WIDE),
        sems(3), sems(3),
        sems(2), sems(2), sems(8), sems(8), sems(32), sems(32),
        sems(2), sems(2), sems(8), sems(8), sems(32), sems(32), sems(32), sems(32),
    ]
    out, dq, dk, dv, dw = pl.pallas_call(
        kernel,
        out_shape=[shape((ROWS, WIDE), BF16)] * 4 + [shape((16, WIDE), F32)],
        in_specs=[anywhere] * 6,
        out_specs=[vmem] * 5,
        scratch_shapes=scratch,
        compiler_params=pltpu.CompilerParams(
            collective_id=0, has_side_effects=True, vmem_limit_bytes=54_800_000
        ),
    )(queries, keys, values, w_out, d_out, slide_lengths)
    out, dq, dk, dv, dw = pl.pallas_call(
        finish,
        out_shape=[shape((ROWS, WIDE), BF16)] * 4 + [shape((12, WIDE), F32)],
        in_specs=[anywhere] * 4 + [vmem],
        out_specs=[anywhere] * 4 + [vmem],
        scratch_shapes=[sems(4)],
        compiler_params=pltpu.CompilerParams(vmem_limit_bytes=4 * 1024 * 1024),
    )(out, dq, dk, dv, dw)
    return out, dq, dk, dv, dw.T


def solution(mesh):
    both = P("seq", "head")
    return jax.shard_map(
        shards,
        mesh=mesh,
        in_specs=(both, both, both, P("head", None), both, P()),
        out_specs=(both, both, both, both, P("head", "seq")),
        check_vma=False,
    )
```
